128 devices in a mesh: dp: 1, sp: 64 (over z, y, x), tp: 2 (over core).
Axes of the slice: x: 4, y: 4, z: 4, core: 2. Of those that a mesh axis runs over, the one named last changes fastest.
Arguments:
- tokens: bfloat16 [131072, 2688], P(('dp', 'sp', 'tp'))
- w_in: bfloat16 [2688, 10304], P(None, 'tp')
- conv_w: bfloat16 [4, 8, 768], P(None, 'tp')
- conv_bias: bfloat16 [8, 768], P('tp')
- a_log: float32 [64], P('tp')
- dt_bias: float32 [64], P('tp')
- d_skip: float32 [64], P('tp')
- norm_w: bfloat16 [4096], P('tp')
- w_out: bfloat16 [4096, 2688], P('tp')
Outputs:
- output: bfloat16 [131072, 2688], P(('dp', 'sp', 'tp'))
All inputs are finite; a program needn't handle non-finite values.
Results may differ from the reference program's by a relative error of at most 0.0146417.
Values are sent between devices in bfloat16 or wider.
A program may use at most 1 GiB of HBM per device.

```python
import jax
import jax.numpy as jnp
from jax import lax

SEQ_LEN = 131072
BLOCK_LEN = 2048
D_MODEL = 2688
N_HEADS = 64
HEAD_DIM = 64
STATE_DIM = 128
GROUPS = 8
TP_SHARDS = 2
SEG_LEN = 256
CONV_TAPS = 4

INNER_DIM = N_HEADS * HEAD_DIM
HEAD_REP = N_HEADS // GROUPS
GROUP_INNER = INNER_DIM // GROUPS
CONV_COLS = GROUP_INNER + 2 * STATE_DIM
GROUP_COLS = 2 * GROUP_INNER + 2 * STATE_DIM + HEAD_REP
SHARD_INNER = INNER_DIM // TP_SHARDS
NORM_EPS = 1e-5


def setup_inputs(seed: int = 0, part: int = 0) -> dict:
    key_list = jax.random.split(jax.random.key(seed), 9)
    fan_scale = D_MODEL ** -0.5
    state_scale = 3.0 * (BLOCK_LEN * STATE_DIM) ** -0.25
    group_scale = jnp.concatenate([
        jnp.full((2 * GROUP_INNER,), fan_scale, jnp.float32),
        jnp.full((2 * STATE_DIM,), fan_scale * state_scale, jnp.float32),
        jnp.full((HEAD_REP,), 0.5 * fan_scale, jnp.float32)])
    bias_scale = jnp.concatenate([
        jnp.full((GROUP_INNER,), 0.3, jnp.float32),
        jnp.full((2 * STATE_DIM,), 0.3 * state_scale, jnp.float32)])
    tokens = jax.random.normal(jax.random.fold_in(key_list[0], part), (SEQ_LEN, D_MODEL), jnp.float32)
    w_in = jax.random.normal(key_list[1], (D_MODEL, GROUPS * GROUP_COLS), jnp.float32) * jnp.tile(group_scale, GROUPS)
    conv_w = 0.5 * jax.random.normal(key_list[2], (CONV_TAPS, GROUPS, CONV_COLS), jnp.float32)
    conv_bias = jax.random.normal(key_list[3], (GROUPS, CONV_COLS), jnp.float32) * bias_scale
    a_log = jnp.log(jax.random.uniform(key_list[4], (N_HEADS,), jnp.float32, 0.5, 2.0) / BLOCK_LEN)
    dt_bias = jax.random.uniform(key_list[5], (N_HEADS,), jnp.float32, -1.0, 0.5)
    d_skip = jax.random.uniform(key_list[6], (N_HEADS,), jnp.float32, 0.5, 1.5)
    norm_w = jax.random.uniform(key_list[7], (INNER_DIM,), jnp.float32, 0.5, 1.5)
    w_out = jax.random.normal(key_list[8], (INNER_DIM, D_MODEL), jnp.float32) * INNER_DIM ** -0.5
    return {
        "tokens": tokens.astype(jnp.bfloat16),
        "w_in": w_in.astype(jnp.bfloat16),
        "conv_w": conv_w.astype(jnp.bfloat16),
        "conv_bias": conv_bias.astype(jnp.bfloat16),
        "a_log": a_log,
        "dt_bias": dt_bias,
        "d_skip": d_skip,
        "norm_w": norm_w.astype(jnp.bfloat16),
        "w_out": w_out.astype(jnp.bfloat16),
    }


def reference(tokens, w_in, conv_w, conv_bias, a_log, dt_bias, d_skip, norm_w, w_out):
    n_segs = SEQ_LEN // SEG_LEN
    tok_segs = tokens.reshape(n_segs, SEG_LEN, D_MODEL)
    decay_rate = jnp.exp(a_log)
    conv_wf = conv_w.astype(jnp.float32)
    conv_bf = conv_bias.astype(jnp.float32)
    norm_gain = norm_w.astype(jnp.float32).reshape(GROUPS, GROUP_INNER)
    causal = jnp.arange(SEG_LEN)[:, None] >= jnp.arange(SEG_LEN)[None, :]

    def scan_step(carry_in, x_seg):
        conv_tail, ssm_state = carry_in
        projected = jnp.dot(x_seg, w_in, preferred_element_type=jnp.float32).astype(jnp.bfloat16)
        projected = projected.reshape(SEG_LEN, GROUPS, GROUP_COLS)
        gate_z = projected[:, :, :GROUP_INNER]
        conv_in = projected[:, :, GROUP_INNER:GROUP_INNER + CONV_COLS]
        dt_raw = projected[:, :, GROUP_INNER + CONV_COLS:]
        padded = jnp.concatenate([conv_tail, conv_in], axis=0).astype(jnp.float32)
        conv_acc = conv_bf + padded[:SEG_LEN] * conv_wf[0]
        for tap_idx in range(1, CONV_TAPS):
            conv_acc = conv_acc + padded[tap_idx:tap_idx + SEG_LEN] * conv_wf[tap_idx]
        activated = jax.nn.silu(conv_acc).astype(jnp.bfloat16).astype(jnp.float32)
        x_heads = activated[:, :, :GROUP_INNER].reshape(SEG_LEN, N_HEADS, HEAD_DIM)
        b_heads = jnp.repeat(activated[:, :, GROUP_INNER:GROUP_INNER + STATE_DIM], HEAD_REP, axis=1)
        c_heads = jnp.repeat(activated[:, :, GROUP_INNER + STATE_DIM:], HEAD_REP, axis=1)
        dt_step = jax.nn.softplus(dt_raw.astype(jnp.float32).reshape(SEG_LEN, N_HEADS) + dt_bias)
        cum_log = jnp.cumsum(-decay_rate * dt_step, axis=0)
        seg_log = cum_log[:, None, :] - cum_log[None, :, :]
        weights = jnp.exp(jnp.where(causal[:, :, None], seg_log, -jnp.inf))
        scores = jnp.einsum("qhn,vhn->qvh", c_heads, b_heads) * weights * dt_step[None, :, :]
        y_ssd = jnp.einsum("qvh,vhp->qhp", scores, x_heads)
        y_ssd = y_ssd + jnp.exp(cum_log)[:, :, None] * jnp.einsum("qhn,hpn->qhp", c_heads, ssm_state)
        y_ssd = y_ssd + d_skip[None, :, None] * x_heads
        end_w = jnp.exp(cum_log[-1][None, :] - cum_log) * dt_step
        new_state = jnp.exp(cum_log[-1])[:, None, None] * ssm_state + jnp.einsum("vhp,vhn->hpn", x_heads * end_w[:, :, None], b_heads)
        y_gated = y_ssd.reshape(SEG_LEN, GROUPS, GROUP_INNER) * jax.nn.silu(gate_z.astype(jnp.float32))
        inv_rms = lax.rsqrt(jnp.mean(y_gated * y_gated, axis=-1, keepdims=True) + NORM_EPS)
        y_normed = (y_gated * inv_rms * norm_gain).astype(jnp.bfloat16).reshape(SEG_LEN, INNER_DIM)
        part_sum = x_seg.astype(jnp.float32)
        for shard_idx in range(TP_SHARDS):
            lo_row = shard_idx * SHARD_INNER
            shard_out = jnp.dot(y_normed[:, lo_row:lo_row + SHARD_INNER], w_out[lo_row:lo_row + SHARD_INNER], preferred_element_type=jnp.float32)
            part_sum = part_sum + shard_out.astype(jnp.bfloat16).astype(jnp.float32)
        return (conv_in[SEG_LEN - CONV_TAPS + 1:], new_state), part_sum.astype(jnp.bfloat16)

    init_carry = (jnp.zeros((CONV_TAPS - 1, GROUPS, CONV_COLS), jnp.bfloat16), jnp.zeros((N_HEADS, HEAD_DIM, STATE_DIM), jnp.float32))
    scanned = lax.scan(scan_step, init_carry, tok_segs)
    return scanned[1].reshape(SEQ_LEN, D_MODEL)
```

```python
import functools

import jax
import jax.numpy as jnp
from jax import lax
from jax.experimental import pallas as pl
from jax.experimental.pallas import tpu as pltpu
from jax.sharding import PartitionSpec as P

SEG = 128
NORM_EPS = 1e-5
LANES = 128
PIECE_PAD = 8
LOG2E = 1.4426950408889634
F32 = jnp.float32
BF16 = jnp.bfloat16


def spread(values, one_hot):
    n_heads = LANES // 4
    high = values.astype(BF16)
    rest = values - high.astype(F32)
    mid = rest.astype(BF16)
    low = (rest - mid.astype(F32)).astype(BF16)
    lane = lax.broadcasted_iota(jnp.int32, values.shape, 1)
    parts = jnp.where(lane < n_heads, high.astype(F32), jnp.where(lane < 2 * n_heads, mid.astype(F32), low.astype(F32)))
    parts = jnp.where(lane < 3 * n_heads, parts, 0.0).astype(BF16)
    return jnp.dot(parts, one_hot, preferred_element_type=F32)


def conv_kernel(dims, tp_ref, own_ref, oth_ref, halo_ref, cw_ref, cb_ref, hp_ref, oh_ref,
                z_ref, act_ref, dts_ref, end_ref, ext, state, total):
    n_groups, group_inner, n_state, head_rep, half_segs, n_segs = dims
    conv_cols = group_inner + 2 * n_state
    group_cols = 2 * group_inner + 2 * n_state + head_rep
    seg_idx = pl.program_id(0)
    is_own = (seg_idx // half_segs) == tp_ref[0]

    @pl.when(seg_idx == 0)
    def _():
        state[...] = jnp.zeros_like(state)
        total[...] = jnp.zeros_like(total)
        for g in range(n_groups):
            lo = g * group_cols + group_inner
            ext[g, 0:8] = halo_ref[:, lo:lo + conv_cols].astype(F32)[-8:]

    def rows(lo, width):
        return jnp.where(is_own, own_ref[:, lo:lo + width], oth_ref[:, lo:lo + width])

    dt_raw = jnp.concatenate([rows(g * group_cols + group_cols - head_rep, head_rep).astype(F32) for g in range(n_groups)], axis=1)
    dt_raw = jnp.concatenate([dt_raw] * 4, axis=1)
    dt_step = jax.nn.softplus(dt_raw + hp_ref[1:2])
    log_decay = -jnp.exp(hp_ref[0:1]) * dt_step * LOG2E
    row_id = lax.broadcasted_iota(jnp.int32, (SEG, SEG), 0)
    col_id = lax.broadcasted_iota(jnp.int32, (SEG, SEG), 1)
    tri = (row_id >= col_id).astype(F32)
    cum = jnp.dot(tri, log_decay, precision=lax.Precision.HIGHEST, preferred_element_type=F32)
    dts_ref[0] = dt_step
    dts_ref[1] = cum
    seg_total = cum[SEG - 1:SEG]
    total[...] += seg_total
    end_w = spread(jnp.exp2(seg_total - cum) * dt_step, oh_ref[...])
    seg_decay = spread(jnp.exp2(jnp.broadcast_to(seg_total, (8, LANES))), oh_ref[...])[0:1]

    for g in range(n_groups):
        lo = g * group_cols
        z_ref[:, g * group_inner:(g + 1) * group_inner] = rows(lo, group_inner)
        ext[g, 8:8 + SEG] = rows(lo + group_inner, conv_cols).astype(F32)
        c0 = g * conv_cols
        acc = cb_ref[:, c0:c0 + conv_cols] + ext[g, 5:5 + SEG] * cw_ref[0:1, c0:c0 + conv_cols]
        for k in range(1, 4):
            acc = acc + ext[g, 5 + k:5 + k + SEG] * cw_ref[k:k + 1, c0:c0 + conv_cols]
        ext[g, 0:8] = ext[g, SEG:SEG + 8]
        act = (acc / (1.0 + jnp.exp(-acc))).astype(BF16)
        act_ref[:, c0:c0 + conv_cols] = act
        i0, i1 = g * group_inner, (g + 1) * group_inner
        weighted = (act[:, :group_inner].astype(F32) * end_w[:, i0:i1]).astype(BF16)
        b_mat = act[:, group_inner:group_inner + n_state]
        new = lax.dot_general(b_mat, weighted, (((0,), (0,)), ((), ())), preferred_element_type=F32)
        state[:, i0:i1] = state[:, i0:i1] * seg_decay[:, i0:i1] + new

    @pl.when(seg_idx == n_segs - 1)
    def _():
        decay = spread(jnp.exp2(jnp.broadcast_to(total[...], (8, LANES))), oh_ref[...])
        n_tiles = n_groups * group_inner // LANES
        quarters = end_ref.shape[0] // n_tiles
        depth = n_state // quarters
        for t in range(n_tiles):
            for q in range(quarters):
                end_ref[t * quarters + q, 0:depth] = state[q * depth:(q + 1) * depth, t * LANES:(t + 1) * LANES]
                end_ref[t * quarters + q, depth:depth + PIECE_PAD] = decay[:, t * LANES:(t + 1) * LANES]


def exchange_kernel(sp_size, depth, end_ref, in_ref, gathered, starts, recv, send_sem, recv_sem, send_sem2, recv_sem2):
    me = lax.axis_index("sp")
    barrier = pltpu.get_barrier_semaphore()

    def greet(k, carry):
        peer = lax.rem(me + k, sp_size)
        pl.semaphore_signal(barrier, inc=1, device_id={"sp": peer}, device_id_type=pl.DeviceIdType.MESH)
        return carry

    lax.fori_loop(1, sp_size, greet, 0)
    pl.semaphore_wait(barrier, sp_size - 1)

    def send_out(k, carry):
        peer = lax.rem(me + k, sp_size)
        pltpu.make_async_remote_copy(
            src_ref=end_ref.at[peer], dst_ref=gathered.at[me], send_sem=send_sem, recv_sem=recv_sem,
            device_id={"sp": peer}, device_id_type=pl.DeviceIdType.MESH).start()
        return carry

    lax.fori_loop(1, sp_size, send_out, 0)
    others = pl.ds(0, sp_size - 1)
    all_out = pltpu.make_async_copy(end_ref.at[others], gathered.at[others], recv_sem)
    all_out.wait()
    pltpu.make_async_copy(end_ref.at[others], gathered.at[others], send_sem).wait()
    gathered[me] = end_ref[me]

    def scan_step(j, carry):
        starts[j] = carry
        return gathered[j, depth:depth + 1] * carry + gathered[j, 0:depth]

    lax.fori_loop(0, sp_size, scan_step, jnp.zeros((depth, LANES), F32))

    def send_back(k, carry):
        peer = lax.rem(me + k, sp_size)
        pltpu.make_async_remote_copy(
            src_ref=starts.at[peer], dst_ref=recv.at[me], send_sem=send_sem2, recv_sem=recv_sem2,
            device_id={"sp": peer}, device_id_type=pl.DeviceIdType.MESH).start()
        return carry

    lax.fori_loop(1, sp_size, send_back, 0)
    pltpu.make_async_copy(starts.at[others], recv.at[others], recv_sem2).wait()
    pltpu.make_async_copy(starts.at[others], recv.at[others], send_sem2).wait()
    recv[me] = starts[me]
    in_ref[...] = recv[...]


def ssd_kernel(dims, tp_ref, act_ref, z_ref, dts_ref, in_ref, hp_ref, oh_ref, ch_ref, o_ref, state):
    n_groups, group_inner, n_state, head_rep, half_segs, n_segs = dims
    conv_cols = group_inner + 2 * n_state
    n_heads = n_groups * head_rep
    seg_idx = pl.program_id(0)

    @pl.when(seg_idx == 0)
    def _():
        n_tiles = n_groups * group_inner // LANES
        quarters = in_ref.shape[0] // n_tiles
        depth = n_state // quarters
        for t in range(n_tiles):
            for q in range(quarters):
                state[q * depth:(q + 1) * depth, t * LANES:(t + 1) * LANES] = in_ref[t * quarters + q]

    dt_step = dts_ref[0]
    cum = dts_ref[1]
    seg_total = cum[SEG - 1:SEG]
    end_w = spread(jnp.exp2(seg_total - cum) * dt_step, oh_ref[...])
    from_start = spread(jnp.exp2(cum), oh_ref[...])
    seg_decay = from_start[SEG - 1:SEG]
    lane = lax.broadcasted_iota(jnp.int32, (SEG, LANES), 1)
    flipped = jnp.where(lane < n_heads, cum, dt_step).T
    row_id = lax.broadcasted_iota(jnp.int32, (SEG, SEG), 0)
    causal = row_id >= lane
    first_half = lane < LANES // 2

    for g in range(n_groups):
        c0 = g * conv_cols
        i0, i1 = g * group_inner, (g + 1) * group_inner
        x_mat = act_ref[:, c0:c0 + group_inner]
        b_mat = act_ref[:, c0 + group_inner:c0 + group_inner + n_state]
        c_mat = act_ref[:, c0 + group_inner + n_state:c0 + conv_cols]
        c_dot_b = lax.dot_general(c_mat, b_mat, (((1,), (1,)), ((), ())), preferred_element_type=F32)
        diag = []
        for pair in range(head_rep // 2):
            scores = []
            for h in (g * head_rep + 2 * pair, g * head_rep + 2 * pair + 1):
                gap = cum[:, h:h + 1] - flipped[h:h + 1]
                weights = jnp.where(causal, jnp.exp2(gap), 0.0)
                scores.append((c_dot_b * weights * flipped[n_heads + h:n_heads + h + 1]).astype(BF16))
            x_pair = x_mat[:, pair * LANES:(pair + 1) * LANES]
            zero = jnp.zeros_like(x_pair)
            x_both = jnp.concatenate([jnp.where(first_half, x_pair, zero), jnp.where(first_half, zero, x_pair)], axis=0)
            diag.append(jnp.dot(jnp.concatenate(scores, axis=1), x_both, preferred_element_type=F32))
        y_diag = jnp.concatenate(diag, axis=1)
        held = state[:, i0:i1]
        y_off = jnp.dot(c_mat, held.astype(BF16), preferred_element_type=F32) * from_start[:, i0:i1]
        x_wide = x_mat.astype(F32)
        y_ssd = y_diag + y_off + ch_ref[0:1, i0:i1] * x_wide
        weighted = (x_wide * end_w[:, i0:i1]).astype(BF16)
        new = lax.dot_general(b_mat, weighted, (((0,), (0,)), ((), ())), preferred_element_type=F32)
        state[:, i0:i1] = held * seg_decay[:, i0:i1] + new
        gate = z_ref[:, i0:i1].astype(F32)
        gated = y_ssd * (gate / (1.0 + jnp.exp(-gate)))
        inv_rms = lax.rsqrt(jnp.mean(gated * gated, axis=-1, keepdims=True) + NORM_EPS)
        o_ref[0, :, i0:i1] = (gated * inv_rms * ch_ref[1:2, i0:i1]).astype(BF16)


def solution(mesh):
    sp_size, tp_size = mesh.shape["sp"], mesh.shape["tp"]
    row_spec = P(("dp", "sp", "tp"), None)
    swap = [(0, 1), (1, 0)]

    def layer_block(tokens, w_in, conv_w, conv_bias, a_log, dt_bias, d_skip, norm_w, w_out):
        n_groups, conv_cols = conv_bias.shape
        n_heads = a_log.shape[0]
        inner_dim = norm_w.shape[0]
        head_rep = n_heads // n_groups
        group_inner = inner_dim // n_groups
        head_dim = inner_dim // n_heads
        n_state = (conv_cols - group_inner) // 2
        half = tokens.shape[0]
        half_segs = half // SEG
        n_segs = 2 * half_segs
        dims = (n_groups, group_inner, n_state, head_rep, half_segs, n_segs)
        all_cols = w_in.shape[1]
        tp_idx = lax.axis_index("tp")
        tp_arr = tp_idx.reshape(1).astype(jnp.int32)

        other = lax.ppermute(tokens, "tp", swap)
        proj_own = jnp.dot(tokens, w_in, preferred_element_type=F32).astype(BF16)
        proj_oth = jnp.dot(other, w_in, preferred_element_type=F32).astype(BF16)
        tail = jnp.where(tp_idx == 1, proj_own[half - 8:], proj_oth[half - 8:])
        halo = lax.ppermute(tail, "sp", [(i, i + 1) for i in range(sp_size - 1)])

        head_par = jnp.concatenate([jnp.tile(a_log, 4)[None], jnp.tile(dt_bias, 4)[None]], axis=0)
        chan_par = jnp.stack([jnp.repeat(d_skip, head_dim), norm_w.astype(F32)])
        head_of = jnp.arange(inner_dim) // head_dim
        lane_head = jnp.where(jnp.arange(LANES) < 3 * n_heads, jnp.arange(LANES) % n_heads, -1)
        one_hot = (lane_head[:, None] == head_of[None, :]).astype(BF16)

        n_pieces = sp_size
        depth = n_state * inner_dim // LANES // n_pieces
        conv = pl.pallas_call(
            functools.partial(conv_kernel, dims),
            grid_spec=pltpu.PrefetchScalarGridSpec(
                num_scalar_prefetch=1, grid=(n_segs,),
                in_specs=[
                    pl.BlockSpec((SEG, all_cols), lambda i, tp: (jnp.where(i // half_segs == tp[0], i % half_segs, half_segs - 1), 0)),
                    pl.BlockSpec((SEG, all_cols), lambda i, tp: (jnp.where(i // half_segs == tp[0], half_segs - 1, i % half_segs), 0)),
                    pl.BlockSpec((8, all_cols), lambda i, tp: (0, 0)),
                    pl.BlockSpec((4, n_groups * conv_cols), lambda i, tp: (0, 0)),
                    pl.BlockSpec((1, n_groups * conv_cols), lambda i, tp: (0, 0)),
                    pl.BlockSpec((2, LANES), lambda i, tp: (0, 0)),
                    pl.BlockSpec((LANES, inner_dim), lambda i, tp: (0, 0)),
                ],
                out_specs=[
                    pl.BlockSpec((SEG, inner_dim), lambda i, tp: (i, 0)),
                    pl.BlockSpec((SEG, n_groups * conv_cols), lambda i, tp: (i, 0)),
                    pl.BlockSpec((2, SEG, LANES), lambda i, tp: (0, i, 0)),
                    pl.BlockSpec((n_pieces, depth + PIECE_PAD, LANES), lambda i, tp: (0, 0, 0)),
                ],
                scratch_shapes=[
                    pltpu.VMEM((n_groups, SEG + 8, conv_cols), F32),
                    pltpu.VMEM((n_state, inner_dim), F32),
                    pltpu.VMEM((1, LANES), F32),
                ]),
            out_shape=[
                jax.ShapeDtypeStruct((2 * half, inner_dim), BF16),
                jax.ShapeDtypeStruct((2 * half, n_groups * conv_cols), BF16),
                jax.ShapeDtypeStruct((2, 2 * half, LANES), F32),
                jax.ShapeDtypeStruct((n_pieces, depth + PIECE_PAD, LANES), F32),
            ],
            compiler_params=pltpu.CompilerParams(vmem_limit_bytes=48 * 2**20),
            name="conv_states",
        )
        gate_z, act, dts, end_state = conv(
            tp_arr, proj_own, proj_oth, halo, conv_w.reshape(4, n_groups * conv_cols).astype(F32),
            conv_bias.reshape(1, n_groups * conv_cols).astype(F32), head_par, one_hot)

        incoming = pl.pallas_call(
            functools.partial(exchange_kernel, sp_size, depth),
            out_shape=jax.ShapeDtypeStruct((n_pieces, depth, LANES), F32),
            in_specs=[pl.BlockSpec(memory_space=pltpu.VMEM)],
            out_specs=pl.BlockSpec(memory_space=pltpu.VMEM),
            scratch_shapes=[
                pltpu.VMEM((n_pieces, depth + PIECE_PAD, LANES), F32),
                pltpu.VMEM((n_pieces, depth, LANES), F32),
                pltpu.VMEM((n_pieces, depth, LANES), F32),
                pltpu.SemaphoreType.DMA, pltpu.SemaphoreType.DMA,
                pltpu.SemaphoreType.DMA, pltpu.SemaphoreType.DMA,
            ],
            compiler_params=pltpu.CompilerParams(collective_id=0, has_side_effects=True),
            name="state_exchange",
        )(end_state)

        out_rows = pl.pallas_call(
            functools.partial(ssd_kernel, dims),
            grid_spec=pltpu.PrefetchScalarGridSpec(
                num_scalar_prefetch=1, grid=(n_segs,),
                in_specs=[
                    pl.BlockSpec((SEG, n_groups * conv_cols), lambda i, tp: (i, 0)),
                    pl.BlockSpec((SEG, inner_dim), lambda i, tp: (i, 0)),
                    pl.BlockSpec((2, SEG, LANES), lambda i, tp: (0, i, 0)),
                    pl.BlockSpec((n_pieces, depth, LANES), lambda i, tp: (0, 0, 0)),
                    pl.BlockSpec((2, LANES), lambda i, tp: (0, 0)),
                    pl.BlockSpec((LANES, inner_dim), lambda i, tp: (0, 0)),
                    pl.BlockSpec((2, inner_dim), lambda i, tp: (0, 0)),
                ],
                out_specs=pl.BlockSpec((1, SEG, inner_dim), lambda i, tp: (jnp.where(i // half_segs == tp[0], 0, 1), i % half_segs, 0)),
                scratch_shapes=[pltpu.VMEM((n_state, inner_dim), F32)]),
            out_shape=jax.ShapeDtypeStruct((2, half, inner_dim), BF16),
            compiler_params=pltpu.CompilerParams(vmem_limit_bytes=48 * 2**20),
            name="ssd_gate_norm",
        )(tp_arr, act, gate_z, dts, incoming, head_par, one_hot, chan_par)

        part_oth = jnp.dot(out_rows[1], w_out, preferred_element_type=F32).astype(BF16)
        received = lax.ppermute(part_oth, "tp", swap)
        part_own = lax.reduce_precision(jnp.dot(out_rows[0], w_out, preferred_element_type=F32), 8, 7)
        return (tokens.astype(F32) + part_own + received.astype(F32)).astype(BF16)

    return jax.shard_map(
        layer_block,
        mesh=mesh,
        in_specs=(row_spec, P(None, "tp"), P(None, "tp", None), P("tp", None), P("tp"), P("tp"), P("tp"), P("tp"), P("tp", None)),
        out_specs=row_spec,
        check_vma=False)
```

```python
import functools

import jax
import jax.numpy as jnp
from jax import lax
from jax.experimental import pallas as pl
from jax.experimental.pallas import tpu as pltpu
from jax.sharding import PartitionSpec as P

SEG = 128
SUB = 256
HALO = 16
NORM_EPS = 1e-5
LANES = 128
PIECE_PAD = 8
LOG2E = 1.4426950408889634
F32 = jnp.float32
BF16 = jnp.bfloat16


def spread(values, one_hot):
    n_heads = LANES // 4
    high = values.astype(BF16)
    rest = values - high.astype(F32)
    mid = rest.astype(BF16)
    low = (rest - mid.astype(F32)).astype(BF16)
    lane = lax.broadcasted_iota(jnp.int32, values.shape, 1)
    parts = jnp.where(lane < n_heads, high.astype(F32), jnp.where(lane < 2 * n_heads, mid.astype(F32), low.astype(F32)))
    parts = jnp.where(lane < 3 * n_heads, parts, 0.0).astype(BF16)
    return jnp.dot(parts, one_hot, preferred_element_type=F32)


CONTRACT_LAST = (((1,), (1,)), ((), ()))


def weight_copy(wt_ref, weights, sems, group_id, group_cols, offset):
    rows = weights.shape[1]
    lo = pl.multiple_of(group_id * group_cols + offset, 8)
    slot = lax.rem(group_id, 2)
    return pltpu.make_async_copy(wt_ref.at[pl.ds(lo, rows)], weights.at[slot], sems.at[slot])


def project_conv_kernel(dims, tp_ref, own_ref, oth_ref, halo_ref, wt_ref,
                        cw_ref, cb_ref, hp_ref, oh_ref, act_ref, dts_ref, end_ref,
                        x_buf, weights, w_dt, ext0, ext1, ext2, ext3, state, total, sems, wsems, dsems):
    n_groups, group_inner, n_state, head_rep, half = dims
    group_id, half_id = pl.program_id(0), pl.program_id(1)
    n_heads = n_groups * head_rep
    exts = (ext0, ext1, ext2, ext3)

    def copies(first, second):
        return [
            lambda: pltpu.make_async_copy(halo_ref, x_buf.at[0, pl.ds(0, HALO)], sems.at[0]),
            lambda: pltpu.make_async_copy(first, x_buf.at[0, pl.ds(HALO, half)], sems.at[1]),
            lambda: pltpu.make_async_copy(first.at[pl.ds(half - HALO, HALO)], x_buf.at[1, pl.ds(0, HALO)], sems.at[2]),
            lambda: pltpu.make_async_copy(second, x_buf.at[1, pl.ds(HALO, half)], sems.at[3]),
        ]

    start = (group_id == 0) & (half_id == 0)

    @pl.when(start & (tp_ref[0] == 0))
    def _():
        for c in copies(own_ref, oth_ref):
            c().start()

    @pl.when(start & (tp_ref[0] == 1))
    def _():
        for c in copies(oth_ref, own_ref):
            c().start()

    group_cols = 2 * group_inner + 2 * n_state + head_rep
    dt_copies = [
        pltpu.make_async_copy(wt_ref.at[pl.ds((g + 1) * group_cols - head_rep, head_rep)], w_dt.at[pl.ds(g * head_rep, head_rep)], dsems.at[g])
        for g in range(n_groups)]

    @pl.when(start)
    def _():
        weight_copy(wt_ref, weights, wsems, group_id, group_cols, group_inner).start()
        w_dt[n_heads:LANES] = jnp.zeros((LANES - n_heads, w_dt.shape[1]), BF16)
        for c in dt_copies:
            c.start()
        total[...] = jnp.zeros_like(total)
        for c in dt_copies:
            c.wait()
        for c in copies(own_ref, oth_ref)[:2]:
            c().wait()

    @pl.when((group_id == 0) & (half_id == 1))
    def _():
        for c in copies(own_ref, oth_ref)[2:]:
            c().wait()

    @pl.when(half_id == 0)
    def _():
        weight_copy(wt_ref, weights, wsems, group_id, group_cols, group_inner).wait()
        state[...] = jnp.zeros_like(state)

    @pl.when((half_id == 0) & (group_id < n_groups - 1))
    def _():
        weight_copy(wt_ref, weights, wsems, group_id + 1, group_cols, group_inner).start()

    w_slot = lax.rem(group_id, 2)

    row0 = half_id * half

    @pl.when(group_id == 0)
    def _():
        def step(s, carry):
            at = pl.ds(pl.multiple_of(HALO + s * SUB, 16), SUB)
            raw = lax.dot_general(x_buf[half_id, at, :], w_dt[...], CONTRACT_LAST, preferred_element_type=F32).astype(BF16).astype(F32)
            raw = raw + pltpu.roll(raw, n_heads, 1) + pltpu.roll(raw, 2 * n_heads, 1) + pltpu.roll(raw, 3 * n_heads, 1)
            dt_step = jax.nn.softplus(raw + hp_ref[1:2])
            log_decay = -jnp.exp(hp_ref[0:1]) * dt_step * LOG2E
            row_id = lax.broadcasted_iota(jnp.int32, (SEG, SEG), 0)
            col_id = lax.broadcasted_iota(jnp.int32, (SEG, SEG), 1)
            tri = (row_id >= col_id).astype(F32)
            for q in range(SUB // SEG):
                lo, hi = q * SEG, (q + 1) * SEG
                cum = jnp.dot(tri, log_decay[lo:hi], precision=lax.Precision.HIGHEST, preferred_element_type=F32)
                out = pl.ds(pl.multiple_of(row0 + s * SUB + lo, SEG), SEG)
                dts_ref[0, out, :] = dt_step[lo:hi]
                dts_ref[1, out, :] = cum
                dts_ref[2, out, :] = cum + total[...]
                total[...] += cum[SEG - 1:SEG]
            return carry
        lax.fori_loop(0, half // SUB, step, 0)

    n_cols = weights.shape[1] // LANES

    def matmul(s):
        lo = 0 if s == 0 else HALO
        rows = x_buf[half_id, s * SUB + lo:HALO + (s + 1) * SUB, :]
        raw = lax.dot_general(rows, weights[w_slot], CONTRACT_LAST, preferred_element_type=F32).astype(BF16).astype(F32)
        for t in range(n_cols):
            exts[s][t, lo:HALO + SUB] = raw[:, t * LANES:(t + 1) * LANES]

    def convolved(s, t):
        ext = exts[s]
        if s > 0:
            ext[t, 8:HALO] = exts[s - 1][t, HALO + SUB - 8:HALO + SUB]
        lanes = slice(t * LANES, (t + 1) * LANES)
        acc = cb_ref[:, lanes] + ext[t, HALO - 3:HALO - 3 + SUB] * cw_ref[0:1, lanes]
        for k in range(1, 4):
            acc = acc + ext[t, HALO - 3 + k:HALO - 3 + k + SUB] * cw_ref[k:k + 1, lanes]
        act = (acc / (1.0 + jnp.exp(-acc))).astype(BF16)
        act_ref[s * SUB:(s + 1) * SUB, lanes] = act
        return act

    def vector(s):
        n_x = group_inner // LANES
        b_all = convolved(s, n_x)
        convolved(s, n_x + 1)
        at = pl.ds(pl.multiple_of(row0 + s * SUB, SUB), SUB)
        dt_step, cum = dts_ref[0, at, :], dts_ref[1, at, :]
        ends = [cum[(q + 1) * SEG - 1:(q + 1) * SEG] for q in range(SUB // SEG)]
        last = jnp.concatenate([jnp.broadcast_to(e, (SEG, LANES)) for e in ends], axis=0)
        end_w = spread(jnp.exp2(last - cum) * dt_step, oh_ref[...])
        decay = spread(jnp.exp2(jnp.concatenate([jnp.broadcast_to(e, (8, LANES)) for e in ends], axis=0)), oh_ref[...])
        weighted = [(convolved(s, t).astype(F32) * end_w[:, t * LANES:(t + 1) * LANES]).astype(BF16) for t in range(n_x)]
        weighted = jnp.concatenate(weighted, axis=1)
        for q in range(SUB // SEG):
            lo, hi = q * SEG, (q + 1) * SEG
            new = lax.dot_general(b_all[lo:hi], weighted[lo:hi], (((0,), (0,)), ((), ())), preferred_element_type=F32)
            state[...] = state[...] * decay[8 * q:8 * q + 1] + new

    matmul(0)
    for s in range(1, half // SUB):
        matmul(s)
        vector(s - 1)
    vector(half // SUB - 1)

    @pl.when(half_id == 1)
    def _():
        decay = spread(jnp.exp2(jnp.broadcast_to(total[...], (8, LANES))), oh_ref[...])
        n_tiles = group_inner // LANES
        quarters = end_ref.shape[0] // (n_groups * n_tiles)
        depth = n_state // quarters
        for t in range(n_tiles):
            for q in range(quarters):
                piece = (group_id * n_tiles + t) * quarters + q
                end_ref[piece, 0:depth] = state[q * depth:(q + 1) * depth, t * LANES:(t + 1) * LANES]
                end_ref[piece, depth:depth + PIECE_PAD] = decay[:, t * LANES:(t + 1) * LANES]


def gate_ssd_kernel(dims, sp_size, end_ref, own_ref, oth_ref, wt_ref, act_ref, dts_ref, oh_ref, ds_ref, z_ref, y_ref, in_ref,
                    x_buf, weights, state, gathered, starts, received, xsems, wsems, send_sem, recv_sem, send_sem2, recv_sem2):
    n_groups, group_inner, n_state, head_rep, half = dims
    conv_cols = group_inner + 2 * n_state
    group_cols = 2 * group_inner + 2 * n_state + head_rep
    n_heads = n_groups * head_rep
    depth = starts.shape[1]
    step_id = pl.program_id(0)
    n_z = 2 * n_groups
    me = lax.axis_index("sp")
    others = pl.ds(0, sp_size - 1)
    mesh_id = pl.DeviceIdType.MESH

    def x_copy(k):
        return pltpu.make_async_copy((own_ref, oth_ref)[k], x_buf.at[k], xsems.at[k])

    @pl.when(step_id == 0)
    def _():
        weight_copy(wt_ref, weights, wsems, 0, group_cols, 0).start()
        x_copy(0).start()
        x_copy(1).start()
        barrier = pltpu.get_barrier_semaphore()

        def greet(k, carry):
            pl.semaphore_signal(barrier, inc=1, device_id={"sp": lax.rem(me + k, sp_size)}, device_id_type=mesh_id)
            return carry

        lax.fori_loop(1, sp_size, greet, 0)

    @pl.when(step_id == 1)
    def _():
        pl.semaphore_wait(pltpu.get_barrier_semaphore(), sp_size - 1)

        def send_out(k, carry):
            peer = lax.rem(me + k, sp_size)
            pltpu.make_async_remote_copy(
                src_ref=end_ref.at[peer], dst_ref=gathered.at[me], send_sem=send_sem, recv_sem=recv_sem,
                device_id={"sp": peer}, device_id_type=mesh_id).start()
            return carry

        lax.fori_loop(1, sp_size, send_out, 0)

    @pl.when(step_id == n_z)
    def _():
        pltpu.make_async_copy(end_ref.at[others], gathered.at[others], recv_sem).wait()
        pltpu.make_async_copy(end_ref.at[others], gathered.at[others], send_sem).wait()
        gathered[me] = end_ref[me]

        def scan_step(j, carry):
            starts[j] = carry
            return gathered[j, depth:depth + 1] * carry + gathered[j, 0:depth]

        lax.fori_loop(0, sp_size, scan_step, jnp.zeros((depth, LANES), F32))

        def send_back(k, carry):
            peer = lax.rem(me + k, sp_size)
            pltpu.make_async_remote_copy(
                src_ref=starts.at[peer], dst_ref=received.at[me], send_sem=send_sem2, recv_sem=recv_sem2,
                device_id={"sp": peer}, device_id_type=mesh_id).start()
            return carry

        lax.fori_loop(1, sp_size, send_back, 0)
        state[...] = jnp.zeros_like(state)

    @pl.when(step_id < n_z)
    def _():
        group_id, slot = step_id // 2, lax.rem(step_id, 2)

        @pl.when(slot == 0)
        def _():
            weight_copy(wt_ref, weights, wsems, group_id, group_cols, 0).wait()

        @pl.when((slot == 0) & (group_id < n_groups - 1))
        def _():
            weight_copy(wt_ref, weights, wsems, group_id + 1, group_cols, 0).start()

        for k in range(2):
            @pl.when(step_id == k)
            def _(k=k):
                x_copy(k).wait()

        z_ref[0] = lax.dot_general(x_buf[slot], weights[lax.rem(group_id, 2)], CONTRACT_LAST, preferred_element_type=F32).astype(BF16)

    @pl.when(step_id >= n_z)
    def _():
        dt_step = dts_ref[0]
        cum = dts_ref[1]
        seg_total = cum[SEG - 1:SEG]
        end_w = spread(jnp.exp2(seg_total - cum) * dt_step, oh_ref[...])
        from_start = spread(jnp.exp2(cum), oh_ref[...])
        seg_decay = from_start[SEG - 1:SEG]
        lane = lax.broadcasted_iota(jnp.int32, (SEG, LANES), 1)
        flipped = jnp.where(lane < n_heads, cum, dt_step).T
        row_id = lax.broadcasted_iota(jnp.int32, (SEG, SEG), 0)
        causal = row_id >= lane
        first_half = lane < LANES // 2

        for g in range(n_groups):
            c0 = g * conv_cols
            i0, i1 = g * group_inner, (g + 1) * group_inner
            x_mat = act_ref[:, c0:c0 + group_inner]
            b_mat = act_ref[:, c0 + group_inner:c0 + group_inner + n_state]
            c_mat = act_ref[:, c0 + group_inner + n_state:c0 + conv_cols]
            c_dot_b = lax.dot_general(c_mat, b_mat, (((1,), (1,)), ((), ())), preferred_element_type=F32)
            diag = []
            for pair in range(head_rep // 2):
                scores = []
                for h in (g * head_rep + 2 * pair, g * head_rep + 2 * pair + 1):
                    gap = cum[:, h:h + 1] - flipped[h:h + 1]
                    weights = jnp.where(causal, jnp.exp2(gap), 0.0)
                    scores.append((c_dot_b * weights * flipped[n_heads + h:n_heads + h + 1]).astype(BF16))
                x_pair = x_mat[:, pair * LANES:(pair + 1) * LANES]
                zero = jnp.zeros_like(x_pair)
                x_both = jnp.concatenate([jnp.where(first_half, x_pair, zero), jnp.where(first_half, zero, x_pair)], axis=0)
                diag.append(jnp.dot(jnp.concatenate(scores, axis=1), x_both, preferred_element_type=F32))
            y_diag = jnp.concatenate(diag, axis=1)
            held = state[:, i0:i1]
            y_off = jnp.dot(c_mat, held.astype(BF16), preferred_element_type=F32) * from_start[:, i0:i1]
            x_wide = x_mat.astype(F32)
            y_ref[:, i0:i1] = y_diag + y_off + ds_ref[0:1, i0:i1] * x_wide
            weighted = (x_wide * end_w[:, i0:i1]).astype(BF16)
            new = lax.dot_general(b_mat, weighted, (((0,), (0,)), ((), ())), preferred_element_type=F32)
            state[:, i0:i1] = held * seg_decay[:, i0:i1] + new

    @pl.when(step_id == pl.num_programs(0) - 1)
    def _():
        pltpu.make_async_copy(starts.at[others], received.at[others], recv_sem2).wait()
        pltpu.make_async_copy(starts.at[others], received.at[others], send_sem2).wait()
        received[me] = starts[me]
        in_ref[...] = received[...]


def gate_norm_kernel(dims, tp_ref, y_ref, c0_ref, c1_ref, c2_ref, c3_ref, z_ref, dts_ref, in_ref, oh_ref, nw_ref, o_ref, state):
    n_groups, group_inner, n_state, head_rep, half = dims

    @pl.when(pl.program_id(0) == 0)
    def _():
        n_tiles = n_groups * group_inner // LANES
        quarters = in_ref.shape[0] // n_tiles
        depth = n_state // quarters
        for t in range(n_tiles):
            for q in range(quarters):
                state[q * depth:(q + 1) * depth, t * LANES:(t + 1) * LANES] = in_ref[t * quarters + q].astype(BF16)

    from_start = spread(jnp.exp2(dts_ref[0]), oh_ref[...])
    for g, c_ref in enumerate((c0_ref, c1_ref, c2_ref, c3_ref)):
        i0, i1 = g * group_inner, (g + 1) * group_inner
        y_in = jnp.dot(c_ref[...], state[:, i0:i1], preferred_element_type=F32)
        y_ssd = y_ref[:, i0:i1] + y_in * from_start[:, i0:i1]
        gate = z_ref[0, :, i0:i1].astype(F32)
        gated = y_ssd * (gate / (1.0 + jnp.exp(-gate)))
        inv_rms = lax.rsqrt(jnp.mean(gated * gated, axis=-1, keepdims=True) + NORM_EPS)
        o_ref[:, i0:i1] = (gated * inv_rms * nw_ref[0:1, i0:i1].astype(F32)).astype(BF16)


def solution(mesh):
    sp_size, tp_size = mesh.shape["sp"], mesh.shape["tp"]
    row_spec = P(("dp", "sp", "tp"), None)
    swap = [(0, 1), (1, 0)]

    def layer_block(tokens, w_in, conv_w, conv_bias, a_log, dt_bias, d_skip, norm_w, w_out):
        n_groups, conv_cols = conv_bias.shape
        n_heads = a_log.shape[0]
        inner_dim = norm_w.shape[0]
        head_rep = n_heads // n_groups
        group_inner = inner_dim // n_groups
        head_dim = inner_dim // n_heads
        n_state = (conv_cols - group_inner) // 2
        half, width = tokens.shape
        rows = 2 * half
        all_conv = n_groups * conv_cols
        dims = (n_groups, group_inner, n_state, head_rep, half)
        tp_idx = lax.axis_index("tp")
        tp_arr = tp_idx.reshape(1).astype(jnp.int32)
        any_spec = pl.BlockSpec(memory_space=pl.ANY)
        limit = 60 * 2**20
        w_in_t = w_in.T

        other = lax.ppermute(tokens, "tp", swap)
        tail = tokens[half - HALO:]
        edge = [(2 * i + 1, 2 * i + 2) for i in range(sp_size - 1)]
        edge_same = [(2 * i + 1, 2 * i + 3) for i in range(sp_size - 1)]
        halo = lax.ppermute(tail, ("sp", "tp"), edge) + lax.ppermute(tail, ("sp", "tp"), edge_same)

        head_par = jnp.concatenate([jnp.tile(a_log, 4)[None], jnp.tile(dt_bias, 4)[None]], axis=0)
        skip_row = jnp.repeat(d_skip, head_dim)[None]
        head_of = jnp.arange(inner_dim) // head_dim
        lane_head = jnp.where(jnp.arange(LANES) < 3 * n_heads, jnp.arange(LANES) % n_heads, -1)
        one_hot = (lane_head[:, None] == head_of[None, :]).astype(BF16)
        cw = conv_w.reshape(4, all_conv).astype(F32)
        cb = conv_bias.reshape(1, all_conv).astype(F32)

        n_pieces = sp_size
        depth = n_state * inner_dim // LANES // n_pieces
        once = dict(pipeline_mode=pl.Buffered(buffer_count=1))
        act, dts, end_state = pl.pallas_call(
            functools.partial(project_conv_kernel, dims),
            grid_spec=pltpu.PrefetchScalarGridSpec(
                num_scalar_prefetch=1, grid=(n_groups, 2),
                in_specs=[
                    any_spec, any_spec, any_spec, any_spec,
                    pl.BlockSpec((4, conv_cols), lambda g, i, tp: (0, g)),
                    pl.BlockSpec((1, conv_cols), lambda g, i, tp: (0, g)),
                    pl.BlockSpec((2, LANES), lambda g, i, tp: (0, 0)),
                    pl.BlockSpec((LANES, group_inner), lambda g, i, tp: (0, g)),
                ],
                out_specs=[
                    pl.BlockSpec((half, conv_cols), lambda g, i, tp: (i, g)),
                    pl.BlockSpec((3, rows, LANES), lambda g, i, tp: (0, 0, 0), **once),
                    pl.BlockSpec((n_pieces, depth + PIECE_PAD, LANES), lambda g, i, tp: (0, 0, 0), **once),
                ],
                scratch_shapes=[
                    pltpu.VMEM((2, HALO + half, width), BF16),
                    pltpu.VMEM((2, conv_cols, width), BF16),
                    pltpu.VMEM((LANES, width), BF16),
                    pltpu.VMEM((conv_cols // LANES, HALO + SUB, LANES), F32),
                    pltpu.VMEM((conv_cols // LANES, HALO + SUB, LANES), F32),
                    pltpu.VMEM((conv_cols // LANES, HALO + SUB, LANES), F32),
                    pltpu.VMEM((conv_cols // LANES, HALO + SUB, LANES), F32),
                    pltpu.VMEM((n_state, group_inner), F32),
                    pltpu.VMEM((1, LANES), F32),
                    pltpu.SemaphoreType.DMA((4,)),
                    pltpu.SemaphoreType.DMA((2,)),
                    pltpu.SemaphoreType.DMA((n_groups,)),
                ]),
            out_shape=[
                jax.ShapeDtypeStruct((rows, all_conv), BF16),
                jax.ShapeDtypeStruct((3, rows, LANES), F32),
                jax.ShapeDtypeStruct((n_pieces, depth + PIECE_PAD, LANES), F32),
            ],
            compiler_params=pltpu.CompilerParams(vmem_limit_bytes=limit),
            cost_estimate=pl.CostEstimate(flops=2 * rows * width * all_conv, bytes_accessed=2 * width * all_conv, transcendentals=0),
            name="project_conv_states",
        )(tp_arr, tokens, other, halo, w_in_t, cw, cb, head_par, one_hot)

        n_z = 2 * n_groups

        def seg_at(i):
            return jnp.maximum(i - n_z, 0)

        def z_at(i):
            return jnp.minimum(i, n_z - 1)

        gate_z, y_local, incoming = pl.pallas_call(
            functools.partial(gate_ssd_kernel, dims, sp_size),
            grid=(n_z + rows // SEG,),
            in_specs=[
                pl.BlockSpec((n_pieces, depth + PIECE_PAD, LANES), lambda i: (0, 0, 0), **once),
                any_spec, any_spec, any_spec,
                pl.BlockSpec((SEG, all_conv), lambda i: (seg_at(i), 0)),
                pl.BlockSpec((2, SEG, LANES), lambda i: (0, seg_at(i), 0)),
                pl.BlockSpec((LANES, inner_dim), lambda i: (0, 0), **once),
                pl.BlockSpec((1, inner_dim), lambda i: (0, 0)),
            ],
            out_specs=[
                pl.BlockSpec((1, half, group_inner), lambda i: (lax.rem(z_at(i), 2), 0, z_at(i) // 2)),
                pl.BlockSpec((SEG, inner_dim), lambda i: (seg_at(i), 0)),
                pl.BlockSpec((n_pieces, depth, LANES), lambda i: (0, 0, 0), **once),
            ],
            out_shape=[
                jax.ShapeDtypeStruct((2, half, inner_dim), BF16),
                jax.ShapeDtypeStruct((rows, inner_dim), F32),
                jax.ShapeDtypeStruct((n_pieces, depth, LANES), F32),
            ],
            scratch_shapes=[
                pltpu.VMEM((2, half, width), BF16),
                pltpu.VMEM((2, group_inner, width), BF16),
                pltpu.VMEM((n_state, inner_dim), F32),
                pltpu.VMEM((n_pieces, depth + PIECE_PAD, LANES), F32),
                pltpu.VMEM((n_pieces, depth, LANES), F32),
                pltpu.VMEM((n_pieces, depth, LANES), F32),
                pltpu.SemaphoreType.DMA((2,)),
                pltpu.SemaphoreType.DMA((2,)),
                pltpu.SemaphoreType.DMA, pltpu.SemaphoreType.DMA,
                pltpu.SemaphoreType.DMA, pltpu.SemaphoreType.DMA,
            ],
            compiler_params=pltpu.CompilerParams(vmem_limit_bytes=limit, collective_id=0, has_side_effects=True),
            name="gate_ssd_exchange",
        )(end_state, tokens, other, w_in_t, act, dts, one_hot, skip_row)

        def finish(slot):
            def at(i, tp):
                return ((tp[0] + slot) % 2) * (half // SUB) + i

            def c_spec(g):
                return pl.BlockSpec((SUB, LANES), lambda i, tp: (at(i, tp), 6 * g + 5))

            return pl.pallas_call(
                functools.partial(gate_norm_kernel, dims),
                grid_spec=pltpu.PrefetchScalarGridSpec(
                    num_scalar_prefetch=1, grid=(half // SUB,),
                    in_specs=[
                        pl.BlockSpec((SUB, inner_dim), lambda i, tp: (at(i, tp), 0)),
                        c_spec(0), c_spec(1), c_spec(2), c_spec(3),
                        pl.BlockSpec((1, SUB, inner_dim), lambda i, tp: (slot, i, 0)),
                        pl.BlockSpec((1, SUB, LANES), lambda i, tp: (2, at(i, tp), 0)),
                        pl.BlockSpec((n_pieces, depth, LANES), lambda i, tp: (0, 0, 0)),
                        pl.BlockSpec((LANES, inner_dim), lambda i, tp: (0, 0)),
                        pl.BlockSpec((1, inner_dim), lambda i, tp: (0, 0)),
                    ],
                    out_specs=pl.BlockSpec((SUB, inner_dim), lambda i, tp: (i, 0)),
                    scratch_shapes=[pltpu.VMEM((n_state, inner_dim), BF16)]),
                out_shape=jax.ShapeDtypeStruct((half, inner_dim), BF16),
                compiler_params=pltpu.CompilerParams(vmem_limit_bytes=48 * 2**20),
                cost_estimate=pl.CostEstimate(flops=half * width * inner_dim, bytes_accessed=10 * half * inner_dim, transcendentals=0),
                name="gate_norm",
            )(tp_arr, y_local, act, act, act, act, gate_z, dts, incoming, one_hot, norm_w[None])

        rows_oth = finish(1)
        part_oth = jnp.dot(rows_oth, w_out, preferred_element_type=F32).astype(BF16)
        received = lax.ppermute(part_oth, "tp", swap)
        rows_own = finish(0)
        part_own = lax.reduce_precision(jnp.dot(rows_own, w_out, preferred_element_type=F32), 8, 7)
        return (tokens.astype(F32) + part_own + received.astype(F32)).astype(BF16)

    return jax.shard_map(
        layer_block,
        mesh=mesh,
        in_specs=(row_spec, P(None, "tp"), P(None, "tp", None), P("tp", None), P("tp"), P("tp"), P("tp"), P("tp"), P("tp", None)),
        out_specs=row_spec,
        check_vma=False)
```

```python
import functools

import jax
import jax.numpy as jnp
from jax import lax
from jax.experimental import pallas as pl
from jax.experimental.pallas import tpu as pltpu
from jax.sharding import PartitionSpec as P

SEG = 128
SUB = 256
HALO = 16
EXCHANGE = True
NORM_EPS = 1e-5
LANES = 128
PIECE_PAD = 8
LOG2E = 1.4426950408889634
F32 = jnp.float32
BF16 = jnp.bfloat16


def spread(values, one_hot):
    n_heads = LANES // 4
    high = values.astype(BF16)
    rest = values - high.astype(F32)
    mid = rest.astype(BF16)
    low = (rest - mid.astype(F32)).astype(BF16)
    lane = lax.broadcasted_iota(jnp.int32, values.shape, 1)
    parts = jnp.where(lane < n_heads, high.astype(F32), jnp.where(lane < 2 * n_heads, mid.astype(F32), low.astype(F32)))
    parts = jnp.where(lane < 3 * n_heads, parts, 0.0).astype(BF16)
    return jnp.dot(parts, one_hot, preferred_element_type=F32)


CONTRACT_LAST = (((1,), (1,)), ((), ()))


def weight_copy(wt_ref, weights, sems, group_id, group_cols, offset):
    rows = weights.shape[1]
    lo = pl.multiple_of(group_id * group_cols + offset, 8)
    slot = lax.rem(group_id, 2)
    return pltpu.make_async_copy(wt_ref.at[pl.ds(lo, rows)], weights.at[slot], sems.at[slot])


def project_conv_kernel(dims, tp_ref, own_ref, oth_ref, halo_ref, wt_ref,
                        cw_ref, cb_ref, hp_ref, oh_ref, act_ref, dts_ref, end_ref,
                        x_buf, weights, w_dt, ext0, ext1, ext2, ext3, state, total, sems, wsems, dsems):
    n_groups, group_inner, n_state, head_rep, half = dims
    group_id, half_id = pl.program_id(0), pl.program_id(1)
    n_heads = n_groups * head_rep
    exts = (ext0, ext1, ext2, ext3)

    def copies(first, second):
        return [
            lambda: pltpu.make_async_copy(halo_ref, x_buf.at[0, pl.ds(0, HALO)], sems.at[0]),
            lambda: pltpu.make_async_copy(first, x_buf.at[0, pl.ds(HALO, half)], sems.at[1]),
            lambda: pltpu.make_async_copy(first.at[pl.ds(half - HALO, HALO)], x_buf.at[1, pl.ds(0, HALO)], sems.at[2]),
            lambda: pltpu.make_async_copy(second, x_buf.at[1, pl.ds(HALO, half)], sems.at[3]),
        ]

    start = (group_id == 0) & (half_id == 0)

    @pl.when(start & (tp_ref[0] == 0))
    def _():
        for c in copies(own_ref, oth_ref):
            c().start()

    @pl.when(start & (tp_ref[0] == 1))
    def _():
        for c in copies(oth_ref, own_ref):
            c().start()

    group_cols = 2 * group_inner + 2 * n_state + head_rep
    dt_copies = [
        pltpu.make_async_copy(wt_ref.at[pl.ds((g + 1) * group_cols - head_rep, head_rep)], w_dt.at[pl.ds(g * head_rep, head_rep)], dsems.at[g])
        for g in range(n_groups)]

    @pl.when(start)
    def _():
        weight_copy(wt_ref, weights, wsems, group_id, group_cols, group_inner).start()
        w_dt[n_heads:LANES] = jnp.zeros((LANES - n_heads, w_dt.shape[1]), BF16)
        for c in dt_copies:
            c.start()
        total[...] = jnp.zeros_like(total)
        for c in dt_copies:
            c.wait()
        for c in copies(own_ref, oth_ref)[:2]:
            c().wait()

    @pl.when((group_id == 0) & (half_id == 1))
    def _():
        for c in copies(own_ref, oth_ref)[2:]:
            c().wait()

    @pl.when(half_id == 0)
    def _():
        weight_copy(wt_ref, weights, wsems, group_id, group_cols, group_inner).wait()
        state[...] = jnp.zeros_like(state)

    @pl.when((half_id == 0) & (group_id < n_groups - 1))
    def _():
        weight_copy(wt_ref, weights, wsems, group_id + 1, group_cols, group_inner).start()

    w_slot = lax.rem(group_id, 2)

    row0 = half_id * half

    @pl.when(group_id == 0)
    def _():
        def step(s, carry):
            at = pl.ds(pl.multiple_of(HALO + s * SUB, 16), SUB)
            raw = lax.dot_general(x_buf[half_id, at, :], w_dt[...], CONTRACT_LAST, preferred_element_type=F32).astype(BF16).astype(F32)
            raw = raw + pltpu.roll(raw, n_heads, 1) + pltpu.roll(raw, 2 * n_heads, 1) + pltpu.roll(raw, 3 * n_heads, 1)
            dt_step = jax.nn.softplus(raw + hp_ref[1:2])
            log_decay = -jnp.exp(hp_ref[0:1]) * dt_step * LOG2E
            row_id = lax.broadcasted_iota(jnp.int32, (SEG, SEG), 0)
            col_id = lax.broadcasted_iota(jnp.int32, (SEG, SEG), 1)
            tri = (row_id >= col_id).astype(F32)
            for q in range(SUB // SEG):
                lo, hi = q * SEG, (q + 1) * SEG
                cum = jnp.dot(tri, log_decay[lo:hi], precision=lax.Precision.HIGHEST, preferred_element_type=F32)
                out = pl.ds(pl.multiple_of(row0 + s * SUB + lo, SEG), SEG)
                dts_ref[0, out, :] = dt_step[lo:hi]
                dts_ref[1, out, :] = cum
                dts_ref[2, out, :] = cum + total[...]
                total[...] += cum[SEG - 1:SEG]
            return carry
        lax.fori_loop(0, half // SUB, step, 0)

    n_cols = weights.shape[1] // LANES

    def matmul(s):
        lo = 0 if s == 0 else HALO
        rows = x_buf[half_id, s * SUB + lo:HALO + (s + 1) * SUB, :]
        raw = lax.dot_general(rows, weights[w_slot], CONTRACT_LAST, preferred_element_type=F32).astype(BF16).astype(F32)
        for t in range(n_cols):
            exts[s][t, lo:HALO + SUB] = raw[:, t * LANES:(t + 1) * LANES]

    def convolved(s, t):
        ext = exts[s]
        if s > 0:
            ext[t, 8:HALO] = exts[s - 1][t, HALO + SUB - 8:HALO + SUB]
        lanes = slice(t * LANES, (t + 1) * LANES)
        acc = cb_ref[:, lanes] + ext[t, HALO - 3:HALO - 3 + SUB] * cw_ref[0:1, lanes]
        for k in range(1, 4):
            acc = acc + ext[t, HALO - 3 + k:HALO - 3 + k + SUB] * cw_ref[k:k + 1, lanes]
        act = (acc / (1.0 + jnp.exp(-acc))).astype(BF16)
        act_ref[s * SUB:(s + 1) * SUB, lanes] = act
        return act

    def vector(s):
        n_x = group_inner // LANES
        b_all = convolved(s, n_x)
        convolved(s, n_x + 1)
        at = pl.ds(pl.multiple_of(row0 + s * SUB, SUB), SUB)
        dt_step, cum = dts_ref[0, at, :], dts_ref[1, at, :]
        ends = [cum[(q + 1) * SEG - 1:(q + 1) * SEG] for q in range(SUB // SEG)]
        last = jnp.concatenate([jnp.broadcast_to(e, (SEG, LANES)) for e in ends], axis=0)
        end_w = spread(jnp.exp2(last - cum) * dt_step, oh_ref[...])
        decay = spread(jnp.exp2(jnp.concatenate([jnp.broadcast_to(e, (8, LANES)) for e in ends], axis=0)), oh_ref[...])
        weighted = [(convolved(s, t).astype(F32) * end_w[:, t * LANES:(t + 1) * LANES]).astype(BF16) for t in range(n_x)]
        weighted = jnp.concatenate(weighted, axis=1)
        for q in range(SUB // SEG):
            lo, hi = q * SEG, (q + 1) * SEG
            new = lax.dot_general(b_all[lo:hi], weighted[lo:hi], (((0,), (0,)), ((), ())), preferred_element_type=F32)
            state[...] = state[...] * decay[8 * q:8 * q + 1] + new

    matmul(0)
    for s in range(1, half // SUB):
        matmul(s)
        vector(s - 1)
    vector(half // SUB - 1)

    @pl.when(half_id == 1)
    def _():
        decay = spread(jnp.exp2(jnp.broadcast_to(total[...], (8, LANES))), oh_ref[...])
        n_tiles = group_inner // LANES
        quarters = end_ref.shape[0] // (n_groups * n_tiles)
        depth = n_state // quarters
        for t in range(n_tiles):
            for q in range(quarters):
                piece = (group_id * n_tiles + t) * quarters + q
                end_ref[piece, 0:depth] = state[q * depth:(q + 1) * depth, t * LANES:(t + 1) * LANES]
                end_ref[piece, depth:depth + PIECE_PAD] = decay[:, t * LANES:(t + 1) * LANES]


def gate_ssd_kernel(dims, sp_size, end_ref, own_ref, oth_ref, wt_ref, act_ref, dts_ref, oh_ref, ds_ref, z_ref, y_ref, in_ref,
                    x_buf, weights, state, gathered, starts, received, xsems, wsems, send_sem, recv_sem, send_sem2, recv_sem2):
    n_groups, group_inner, n_state, head_rep, half = dims
    conv_cols = group_inner + 2 * n_state
    group_cols = 2 * group_inner + 2 * n_state + head_rep
    n_heads = n_groups * head_rep
    depth = starts.shape[1]
    step_id = pl.program_id(0)
    n_z = 2 * n_groups
    me = lax.axis_index("sp")
    others = pl.ds(0, sp_size - 1)
    mesh_id = pl.DeviceIdType.MESH

    def x_copy(k):
        return pltpu.make_async_copy((own_ref, oth_ref)[k], x_buf.at[k], xsems.at[k])

    @pl.when(step_id == 0)
    def _():
        weight_copy(wt_ref, weights, wsems, 0, group_cols, 0).start()
        x_copy(0).start()
        x_copy(1).start()
        barrier = pltpu.get_barrier_semaphore()

        def greet(k, carry):
            pl.semaphore_signal(barrier, inc=1, device_id={"sp": lax.rem(me + k, sp_size)}, device_id_type=mesh_id)
            return carry

        lax.fori_loop(1, sp_size, greet, 0)

    @pl.when(step_id == 1)
    def _():
        pl.semaphore_wait(pltpu.get_barrier_semaphore(), sp_size - 1)

        def send_out(k, carry):
            peer = lax.rem(me + k, sp_size)
            pltpu.make_async_remote_copy(
                src_ref=end_ref.at[peer], dst_ref=gathered.at[me], send_sem=send_sem, recv_sem=recv_sem,
                device_id={"sp": peer}, device_id_type=mesh_id).start()
            return carry

        lax.fori_loop(1, sp_size, send_out, 0)

    @pl.when(step_id == n_z)
    def _():
        pltpu.make_async_copy(end_ref.at[others], gathered.at[others], recv_sem).wait()
        pltpu.make_async_copy(end_ref.at[others], gathered.at[others], send_sem).wait()
        gathered[me] = end_ref[me]

        def scan_step(j, carry):
            starts[j] = carry
            return gathered[j, depth:depth + 1] * carry + gathered[j, 0:depth]

        lax.fori_loop(0, sp_size, scan_step, jnp.zeros((depth, LANES), F32))

        def send_back(k, carry):
            peer = lax.rem(me + k, sp_size)
            pltpu.make_async_remote_copy(
                src_ref=starts.at[peer], dst_ref=received.at[me], send_sem=send_sem2, recv_sem=recv_sem2,
                device_id={"sp": peer}, device_id_type=mesh_id).start()
            return carry

        lax.fori_loop(1, sp_size, send_back, 0)
        state[...] = jnp.zeros_like(state)

    @pl.when(step_id < n_z)
    def _():
        group_id, slot = step_id // 2, lax.rem(step_id, 2)

        @pl.when(slot == 0)
        def _():
            weight_copy(wt_ref, weights, wsems, group_id, group_cols, 0).wait()

        @pl.when((slot == 0) & (group_id < n_groups - 1))
        def _():
            weight_copy(wt_ref, weights, wsems, group_id + 1, group_cols, 0).start()

        for k in range(2):
            @pl.when(step_id == k)
            def _(k=k):
                x_copy(k).wait()

        z_ref[0] = lax.dot_general(x_buf[slot], weights[lax.rem(group_id, 2)], CONTRACT_LAST, preferred_element_type=F32).astype(BF16)

    @pl.when(step_id >= n_z)
    def _():
        dt_step = dts_ref[0]
        cum = dts_ref[1]
        seg_total = cum[SEG - 1:SEG]
        end_w = spread(jnp.exp2(seg_total - cum) * dt_step, oh_ref[...])
        from_start = spread(jnp.exp2(cum), oh_ref[...])
        seg_decay = from_start[SEG - 1:SEG]
        lane = lax.broadcasted_iota(jnp.int32, (SEG, LANES), 1)
        flipped = jnp.where(lane < n_heads, cum, dt_step).T
        row_id = lax.broadcasted_iota(jnp.int32, (SEG, SEG), 0)
        causal = row_id >= lane
        first_half = lane < LANES // 2

        for g in range(n_groups):
            c0 = g * conv_cols
            i0, i1 = g * group_inner, (g + 1) * group_inner
            x_mat = act_ref[:, c0:c0 + group_inner]
            b_mat = act_ref[:, c0 + group_inner:c0 + group_inner + n_state]
            c_mat = act_ref[:, c0 + group_inner + n_state:c0 + conv_cols]
            c_dot_b = lax.dot_general(c_mat, b_mat, (((1,), (1,)), ((), ())), preferred_element_type=F32)
            diag = []
            for pair in range(head_rep // 2):
                scores = []
                for h in (g * head_rep + 2 * pair, g * head_rep + 2 * pair + 1):
                    gap = cum[:, h:h + 1] - flipped[h:h + 1]
                    weights = jnp.where(causal, jnp.exp2(gap), 0.0)
                    scores.append((c_dot_b * weights * flipped[n_heads + h:n_heads + h + 1]).astype(BF16))
                x_pair = x_mat[:, pair * LANES:(pair + 1) * LANES]
                zero = jnp.zeros_like(x_pair)
                x_both = jnp.concatenate([jnp.where(first_half, x_pair, zero), jnp.where(first_half, zero, x_pair)], axis=0)
                diag.append(jnp.dot(jnp.concatenate(scores, axis=1), x_both, preferred_element_type=F32))
            y_diag = jnp.concatenate(diag, axis=1)
            held = state[:, i0:i1]
            y_off = jnp.dot(c_mat, held.astype(BF16), preferred_element_type=F32) * from_start[:, i0:i1]
            x_wide = x_mat.astype(F32)
            y_ref[:, i0:i1] = y_diag + y_off + ds_ref[0:1, i0:i1] * x_wide
            weighted = (x_wide * end_w[:, i0:i1]).astype(BF16)
            new = lax.dot_general(b_mat, weighted, (((0,), (0,)), ((), ())), preferred_element_type=F32)
            state[:, i0:i1] = held * seg_decay[:, i0:i1] + new

    @pl.when(step_id == pl.num_programs(0) - 1)
    def _():
        pltpu.make_async_copy(starts.at[others], received.at[others], recv_sem2).wait()
        pltpu.make_async_copy(starts.at[others], received.at[others], send_sem2).wait()
        received[me] = starts[me]
        in_ref[...] = received[...]


def gate_out_kernel(dims, y_ref, c0_ref, c1_ref, c2_ref, c3_ref, z_ref, dts_ref, in_ref, oh_ref, nw_ref, wo_hbm, tok_ref, out_ref,
                    wo_ref, state, o_next, o_prev, parts, received, wsem, send_sems, recv_sems):
    n_groups, group_inner, n_state, head_rep, half = dims
    step_id = pl.program_id(0)
    n_tiles = half // SUB
    peer = {"tp": 1 - lax.axis_index("tp")} if EXCHANGE else None

    def send(k):
        return pltpu.make_async_remote_copy(
            src_ref=parts.at[k], dst_ref=received.at[k], send_sem=send_sems.at[k], recv_sem=recv_sems.at[k],
            device_id=peer, device_id_type=pl.DeviceIdType.MESH)

    def gate_rows():
        from_start = spread(jnp.exp2(dts_ref[0]), oh_ref[...])
        for g, c_ref in enumerate((c0_ref, c1_ref, c2_ref, c3_ref)):
            i0, i1 = g * group_inner, (g + 1) * group_inner
            y_in = jnp.dot(c_ref[...], state[:, i0:i1], preferred_element_type=F32)
            y_ssd = y_ref[:, i0:i1] + y_in * from_start[:, i0:i1]
            gate = z_ref[0, :, i0:i1].astype(F32)
            gated = y_ssd * (gate / (1.0 + jnp.exp(-gate)))
            inv_rms = lax.rsqrt(jnp.mean(gated * gated, axis=-1, keepdims=True) + NORM_EPS)
            o_next[:, i0:i1] = (gated * inv_rms * nw_ref[0:1, i0:i1].astype(F32)).astype(BF16)

    def out_rows():
        parts[jnp.minimum(step_id - 1, n_tiles)] = jnp.dot(o_prev[...], wo_ref[...], preferred_element_type=F32).astype(BF16)

    wo_copy = pltpu.make_async_copy(wo_hbm, wo_ref, wsem)

    @pl.when(step_id == 0)
    def _():
        wo_copy.start()
        if EXCHANGE:
            pl.semaphore_signal(pltpu.get_barrier_semaphore(), inc=1, device_id=peer, device_id_type=pl.DeviceIdType.MESH)
        lane_tiles = n_groups * group_inner // LANES
        quarters = in_ref.shape[0] // lane_tiles
        depth = n_state // quarters
        for t in range(lane_tiles):
            for q in range(quarters):
                state[q * depth:(q + 1) * depth, t * LANES:(t + 1) * LANES] = in_ref[t * quarters + q].astype(BF16)
        gate_rows()
        wo_copy.wait()
        if EXCHANGE:
            pl.semaphore_wait(pltpu.get_barrier_semaphore(), 1)

    @pl.when((step_id > 0) & (step_id < 2 * n_tiles))
    def _():
        out_rows()
        gate_rows()

    @pl.when(step_id == 2 * n_tiles)
    def _():
        out_rows()

    o_prev[...] = o_next[...]

    if EXCHANGE:
        for k in range(n_tiles):
            @pl.when(step_id == k + 1)
            def _(k=k):
                send(k).start()

            @pl.when(step_id == n_tiles + 1 + k)
            def _(k=k):
                send(k).wait_recv()

    @pl.when(step_id > n_tiles)
    def _():
        got = received[jnp.maximum(step_id - n_tiles - 1, 0)]
        out_ref[...] = (tok_ref[...].astype(F32) + parts[n_tiles].astype(F32) + got.astype(F32)).astype(BF16)

    if EXCHANGE:
        @pl.when(step_id == 2 * n_tiles)
        def _():
            for k in range(n_tiles):
                send(k).wait_send()


def solution(mesh):
    sp_size, tp_size = mesh.shape["sp"], mesh.shape["tp"]
    row_spec = P(("dp", "sp", "tp"), None)
    swap = [(0, 1), (1, 0)]

    def layer_block(tokens, w_in, conv_w, conv_bias, a_log, dt_bias, d_skip, norm_w, w_out):
        n_groups, conv_cols = conv_bias.shape
        n_heads = a_log.shape[0]
        inner_dim = norm_w.shape[0]
        head_rep = n_heads // n_groups
        group_inner = inner_dim // n_groups
        head_dim = inner_dim // n_heads
        n_state = (conv_cols - group_inner) // 2
        half, width = tokens.shape
        rows = 2 * half
        all_conv = n_groups * conv_cols
        dims = (n_groups, group_inner, n_state, head_rep, half)
        tp_idx = lax.axis_index("tp")
        tp_arr = tp_idx.reshape(1).astype(jnp.int32)
        any_spec = pl.BlockSpec(memory_space=pl.ANY)
        limit = 60 * 2**20
        w_in_t = w_in.T

        other = lax.ppermute(tokens, "tp", swap)
        tail = tokens[half - HALO:]
        edge = [(2 * i + 1, 2 * i + 2) for i in range(sp_size - 1)]
        edge_same = [(2 * i + 1, 2 * i + 3) for i in range(sp_size - 1)]
        halo = lax.ppermute(tail, ("sp", "tp"), edge) + lax.ppermute(tail, ("sp", "tp"), edge_same)

        head_par = jnp.concatenate([jnp.tile(a_log, 4)[None], jnp.tile(dt_bias, 4)[None]], axis=0)
        skip_row = jnp.repeat(d_skip, head_dim)[None]
        head_of = jnp.arange(inner_dim) // head_dim
        lane_head = jnp.where(jnp.arange(LANES) < 3 * n_heads, jnp.arange(LANES) % n_heads, -1)
        one_hot = (lane_head[:, None] == head_of[None, :]).astype(BF16)
        cw = conv_w.reshape(4, all_conv).astype(F32)
        cb = conv_bias.reshape(1, all_conv).astype(F32)

        n_pieces = sp_size
        depth = n_state * inner_dim // LANES // n_pieces
        once = dict(pipeline_mode=pl.Buffered(buffer_count=1))
        act, dts, end_state = pl.pallas_call(
            functools.partial(project_conv_kernel, dims),
            grid_spec=pltpu.PrefetchScalarGridSpec(
                num_scalar_prefetch=1, grid=(n_groups, 2),
                in_specs=[
                    any_spec, any_spec, any_spec, any_spec,
                    pl.BlockSpec((4, conv_cols), lambda g, i, tp: (0, g)),
                    pl.BlockSpec((1, conv_cols), lambda g, i, tp: (0, g)),
                    pl.BlockSpec((2, LANES), lambda g, i, tp: (0, 0)),
                    pl.BlockSpec((LANES, group_inner), lambda g, i, tp: (0, g)),
                ],
                out_specs=[
                    pl.BlockSpec((half, conv_cols), lambda g, i, tp: (i, g)),
                    pl.BlockSpec((3, rows, LANES), lambda g, i, tp: (0, 0, 0), **once),
                    pl.BlockSpec((n_pieces, depth + PIECE_PAD, LANES), lambda g, i, tp: (0, 0, 0), **once),
                ],
                scratch_shapes=[
                    pltpu.VMEM((2, HALO + half, width), BF16),
                    pltpu.VMEM((2, conv_cols, width), BF16),
                    pltpu.VMEM((LANES, width), BF16),
                    pltpu.VMEM((conv_cols // LANES, HALO + SUB, LANES), F32),
                    pltpu.VMEM((conv_cols // LANES, HALO + SUB, LANES), F32),
                    pltpu.VMEM((conv_cols // LANES, HALO + SUB, LANES), F32),
                    pltpu.VMEM((conv_cols // LANES, HALO + SUB, LANES), F32),
                    pltpu.VMEM((n_state, group_inner), F32),
                    pltpu.VMEM((1, LANES), F32),
                    pltpu.SemaphoreType.DMA((4,)),
                    pltpu.SemaphoreType.DMA((2,)),
                    pltpu.SemaphoreType.DMA((n_groups,)),
                ]),
            out_shape=[
                jax.ShapeDtypeStruct((rows, all_conv), BF16),
                jax.ShapeDtypeStruct((3, rows, LANES), F32),
                jax.ShapeDtypeStruct((n_pieces, depth + PIECE_PAD, LANES), F32),
            ],
            compiler_params=pltpu.CompilerParams(vmem_limit_bytes=limit),
            cost_estimate=pl.CostEstimate(flops=2 * rows * width * all_conv, bytes_accessed=2 * width * all_conv, transcendentals=0),
            name="project_conv_states",
        )(tp_arr, tokens, other, halo, w_in_t, cw, cb, head_par, one_hot)

        n_z = 2 * n_groups

        def seg_at(i):
            return jnp.maximum(i - n_z, 0)

        def z_at(i):
            return jnp.minimum(i, n_z - 1)

        gate_z, y_local, incoming = pl.pallas_call(
            functools.partial(gate_ssd_kernel, dims, sp_size),
            grid=(n_z + rows // SEG,),
            in_specs=[
                pl.BlockSpec((n_pieces, depth + PIECE_PAD, LANES), lambda i: (0, 0, 0), **once),
                any_spec, any_spec, any_spec,
                pl.BlockSpec((SEG, all_conv), lambda i: (seg_at(i), 0)),
                pl.BlockSpec((2, SEG, LANES), lambda i: (0, seg_at(i), 0)),
                pl.BlockSpec((LANES, inner_dim), lambda i: (0, 0), **once),
                pl.BlockSpec((1, inner_dim), lambda i: (0, 0)),
            ],
            out_specs=[
                pl.BlockSpec((1, half, group_inner), lambda i: (lax.rem(z_at(i), 2), 0, z_at(i) // 2)),
                pl.BlockSpec((SEG, inner_dim), lambda i: (seg_at(i), 0)),
                pl.BlockSpec((n_pieces, depth, LANES), lambda i: (0, 0, 0), **once),
            ],
            out_shape=[
                jax.ShapeDtypeStruct((2, half, inner_dim), BF16),
                jax.ShapeDtypeStruct((rows, inner_dim), F32),
                jax.ShapeDtypeStruct((n_pieces, depth, LANES), F32),
            ],
            scratch_shapes=[
                pltpu.VMEM((2, half, width), BF16),
                pltpu.VMEM((2, group_inner, width), BF16),
                pltpu.VMEM((n_state, inner_dim), F32),
                pltpu.VMEM((n_pieces, depth + PIECE_PAD, LANES), F32),
                pltpu.VMEM((n_pieces, depth, LANES), F32),
                pltpu.VMEM((n_pieces, depth, LANES), F32),
                pltpu.SemaphoreType.DMA((2,)),
                pltpu.SemaphoreType.DMA((2,)),
                pltpu.SemaphoreType.DMA, pltpu.SemaphoreType.DMA,
                pltpu.SemaphoreType.DMA, pltpu.SemaphoreType.DMA,
            ],
            compiler_params=pltpu.CompilerParams(vmem_limit_bytes=limit, collective_id=0, has_side_effects=True),
            name="gate_ssd_exchange",
        )(end_state, tokens, other, w_in_t, act, dts, one_hot, skip_row)

        n_tiles = half // SUB

        def tile(i):
            return jnp.minimum(i, 2 * n_tiles - 1)

        def slot_of(i):
            return 1 - tile(i) // n_tiles

        def row_at(i):
            return lax.rem(lax.axis_index("tp") + slot_of(i), 2) * n_tiles + lax.rem(tile(i), n_tiles)

        def own_at(i):
            return jnp.maximum(i - n_tiles - 1, 0)

        def c_spec(g):
            return pl.BlockSpec((SUB, LANES), lambda i: (row_at(i), 6 * g + 5))

        return pl.pallas_call(
            functools.partial(gate_out_kernel, dims),
            grid=(2 * n_tiles + 1,),
            in_specs=[
                pl.BlockSpec((SUB, inner_dim), lambda i: (row_at(i), 0)),
                c_spec(0), c_spec(1), c_spec(2), c_spec(3),
                pl.BlockSpec((1, SUB, inner_dim), lambda i: (slot_of(i), lax.rem(tile(i), n_tiles), 0)),
                pl.BlockSpec((1, SUB, LANES), lambda i: (2, row_at(i), 0)),
                pl.BlockSpec((n_pieces, depth, LANES), lambda i: (0, 0, 0), **once),
                pl.BlockSpec((LANES, inner_dim), lambda i: (0, 0), **once),
                pl.BlockSpec((1, inner_dim), lambda i: (0, 0)),
                any_spec,
                pl.BlockSpec((SUB, width), lambda i: (own_at(i), 0)),
            ],
            out_specs=pl.BlockSpec((SUB, width), lambda i: (own_at(i), 0)),
            out_shape=jax.ShapeDtypeStruct((half, width), BF16),
            scratch_shapes=[
                pltpu.VMEM((inner_dim, width), BF16),
                pltpu.VMEM((n_state, inner_dim), BF16),
                pltpu.VMEM((SUB, inner_dim), BF16),
                pltpu.VMEM((SUB, inner_dim), BF16),
                pltpu.VMEM((n_tiles + 1, SUB, width), BF16),
                pltpu.VMEM((n_tiles, SUB, width), BF16),
                pltpu.SemaphoreType.DMA,
                pltpu.SemaphoreType.DMA((n_tiles,)),
                pltpu.SemaphoreType.DMA((n_tiles,)),
            ],
            compiler_params=pltpu.CompilerParams(vmem_limit_bytes=limit, **(dict(collective_id=1, has_side_effects=True) if EXCHANGE else {})),
            name="gate_out_swap",
        )(y_local, act, act, act, act, gate_z, dts, incoming, one_hot, norm_w[None], w_out, tokens)

    return jax.shard_map(
        layer_block,
        mesh=mesh,
        in_specs=(row_spec, P(None, "tp"), P(None, "tp", None), P("tp", None), P("tp"), P("tp"), P("tp"), P("tp"), P("tp", None)),
        out_specs=row_spec,
        check_vma=False)
```

```python
import functools

import jax
import jax.numpy as jnp
from jax import lax
from jax.experimental import pallas as pl
from jax.experimental.pallas import tpu as pltpu
from jax.sharding import PartitionSpec as P

SEG = 128
SUB = 256
HALO = 16
EXCHANGE = True
NORM_EPS = 1e-5
LANES = 128
PIECE_PAD = 8
LOG2E = 1.4426950408889634
F32 = jnp.float32
BF16 = jnp.bfloat16


def spread(values, one_hot):
    n_heads = LANES // 4
    high = values.astype(BF16)
    rest = values - high.astype(F32)
    mid = rest.astype(BF16)
    low = (rest - mid.astype(F32)).astype(BF16)
    lane = lax.broadcasted_iota(jnp.int32, values.shape, 1)
    parts = jnp.where(lane < n_heads, high.astype(F32), jnp.where(lane < 2 * n_heads, mid.astype(F32), low.astype(F32)))
    parts = jnp.where(lane < 3 * n_heads, parts, 0.0).astype(BF16)
    return jnp.dot(parts, one_hot, preferred_element_type=F32)


CONTRACT_LAST = (((1,), (1,)), ((), ()))


def weight_copy(wt_ref, weights, sems, group_id, group_cols, offset):
    rows = weights.shape[1]
    lo = pl.multiple_of(group_id * group_cols + offset, 8)
    slot = lax.rem(group_id, 2)
    return pltpu.make_async_copy(wt_ref.at[pl.ds(lo, rows)], weights.at[slot], sems.at[slot])


def project_conv_kernel(dims, tp_ref, own_ref, oth_ref, halo_ref, wt_ref,
                        cw_ref, cb_ref, hp_ref, oh_ref, act_ref, dts_ref, end_ref,
                        x_buf, weights, w_dt, ext0, ext1, ext2, ext3, state, total, sems, wsems, dsems):
    n_groups, group_inner, n_state, head_rep, half = dims
    group_id = pl.program_id(0)
    n_heads = n_groups * head_rep
    exts = (ext0, ext1, ext2, ext3)

    def copies(first, second):
        return [
            lambda: pltpu.make_async_copy(halo_ref, x_buf.at[0, pl.ds(0, HALO)], sems.at[0]),
            lambda: pltpu.make_async_copy(first, x_buf.at[0, pl.ds(HALO, half)], sems.at[1]),
            lambda: pltpu.make_async_copy(first.at[pl.ds(half - HALO, HALO)], x_buf.at[1, pl.ds(0, HALO)], sems.at[2]),
            lambda: pltpu.make_async_copy(second, x_buf.at[1, pl.ds(HALO, half)], sems.at[3]),
        ]

    start = group_id == 0

    @pl.when(start & (tp_ref[0] == 0))
    def _():
        for c in copies(own_ref, oth_ref):
            c().start()

    @pl.when(start & (tp_ref[0] == 1))
    def _():
        for c in copies(oth_ref, own_ref):
            c().start()

    group_cols = 2 * group_inner + 2 * n_state + head_rep
    dt_copies = [
        pltpu.make_async_copy(wt_ref.at[pl.ds((g + 1) * group_cols - head_rep, head_rep)], w_dt.at[pl.ds(g * head_rep, head_rep)], dsems.at[g])
        for g in range(n_groups)]

    @pl.when(start)
    def _():
        weight_copy(wt_ref, weights, wsems, group_id, group_cols, group_inner).start()
        w_dt[n_heads:LANES] = jnp.zeros((LANES - n_heads, w_dt.shape[1]), BF16)
        for c in dt_copies:
            c.start()
        total[...] = jnp.zeros_like(total)
        for c in dt_copies:
            c.wait()
        for c in copies(own_ref, oth_ref)[:2]:
            c().wait()

    weight_copy(wt_ref, weights, wsems, group_id, group_cols, group_inner).wait()
    state[...] = jnp.zeros_like(state)

    @pl.when(group_id < n_groups - 1)
    def _():
        weight_copy(wt_ref, weights, wsems, group_id + 1, group_cols, group_inner).start()

    w_slot = lax.rem(group_id, 2)

    def steps_of(half_id):
        def step(s, carry):
            at = pl.ds(pl.multiple_of(HALO + s * SUB, 16), SUB)
            raw = lax.dot_general(x_buf[half_id, at, :], w_dt[...], CONTRACT_LAST, preferred_element_type=F32).astype(BF16).astype(F32)
            raw = raw + pltpu.roll(raw, n_heads, 1) + pltpu.roll(raw, 2 * n_heads, 1) + pltpu.roll(raw, 3 * n_heads, 1)
            dt_step = jax.nn.softplus(raw + hp_ref[1:2])
            log_decay = -jnp.exp(hp_ref[0:1]) * dt_step * LOG2E
            row_id = lax.broadcasted_iota(jnp.int32, (SEG, SEG), 0)
            col_id = lax.broadcasted_iota(jnp.int32, (SEG, SEG), 1)
            tri = (row_id >= col_id).astype(F32)
            for q in range(SUB // SEG):
                lo, hi = q * SEG, (q + 1) * SEG
                cum = jnp.dot(tri, log_decay[lo:hi], precision=lax.Precision.HIGHEST, preferred_element_type=F32)
                out = pl.ds(pl.multiple_of(half_id * half + s * SUB + lo, SEG), SEG)
                dts_ref[0, out, :] = dt_step[lo:hi]
                dts_ref[1, out, :] = cum
                dts_ref[2, out, :] = cum + total[...]
                total[...] += cum[SEG - 1:SEG]
            return carry
        lax.fori_loop(0, half // SUB, step, 0)

    @pl.when(group_id == 0)
    def _():
        steps_of(0)

    n_cols = weights.shape[1] // LANES

    def matmul(half_id, s):
        lo = 0 if s == 0 else HALO
        rows = x_buf[half_id, s * SUB + lo:HALO + (s + 1) * SUB, :]
        raw = lax.dot_general(rows, weights[w_slot], CONTRACT_LAST, preferred_element_type=F32).astype(BF16).astype(F32)
        for t in range(n_cols):
            exts[s][t, lo:HALO + SUB] = raw[:, t * LANES:(t + 1) * LANES]

    def convolved(half_id, s, t):
        ext = exts[s]
        if s > 0:
            ext[t, 8:HALO] = exts[s - 1][t, HALO + SUB - 8:HALO + SUB]
        lanes = slice(t * LANES, (t + 1) * LANES)
        acc = cb_ref[:, lanes] + ext[t, HALO - 3:HALO - 3 + SUB] * cw_ref[0:1, lanes]
        for k in range(1, 4):
            acc = acc + ext[t, HALO - 3 + k:HALO - 3 + k + SUB] * cw_ref[k:k + 1, lanes]
        act = (acc / (1.0 + jnp.exp(-acc))).astype(BF16)
        act_ref[half_id * half + s * SUB:half_id * half + (s + 1) * SUB, lanes] = act
        return act

    def vector(half_id, s):
        n_x = group_inner // LANES
        b_all = convolved(half_id, s, n_x)
        convolved(half_id, s, n_x + 1)
        at = slice(half_id * half + s * SUB, half_id * half + (s + 1) * SUB)
        dt_step, cum = dts_ref[0, at, :], dts_ref[1, at, :]
        ends = [cum[(q + 1) * SEG - 1:(q + 1) * SEG] for q in range(SUB // SEG)]
        last = jnp.concatenate([jnp.broadcast_to(e, (SEG, LANES)) for e in ends], axis=0)
        end_w = spread(jnp.exp2(last - cum) * dt_step, oh_ref[...])
        decay = spread(jnp.exp2(jnp.concatenate([jnp.broadcast_to(e, (8, LANES)) for e in ends], axis=0)), oh_ref[...])
        weighted = [(convolved(half_id, s, t).astype(F32) * end_w[:, t * LANES:(t + 1) * LANES]).astype(BF16) for t in range(n_x)]
        weighted = jnp.concatenate(weighted, axis=1)
        for q in range(SUB // SEG):
            lo, hi = q * SEG, (q + 1) * SEG
            new = lax.dot_general(b_all[lo:hi], weighted[lo:hi], (((0,), (0,)), ((), ())), preferred_element_type=F32)
            state[...] = state[...] * decay[8 * q:8 * q + 1] + new

    order = [(h, s) for h in range(2) for s in range(half // SUB)]
    matmul(*order[0])
    for k in range(1, len(order)):
        if order[k] == (1, 0):
            @pl.when(group_id == 0)
            def _():
                for c in copies(own_ref, oth_ref)[2:]:
                    c().wait()
                steps_of(1)
        matmul(*order[k])
        vector(*order[k - 1])
    vector(*order[-1])

    decay = spread(jnp.exp2(jnp.broadcast_to(total[...], (8, LANES))), oh_ref[...])
    n_tiles = group_inner // LANES
    quarters = end_ref.shape[0] // (n_groups * n_tiles)
    depth = n_state // quarters
    for t in range(n_tiles):
        for q in range(quarters):
            piece = (group_id * n_tiles + t) * quarters + q
            end_ref[piece, 0:depth] = state[q * depth:(q + 1) * depth, t * LANES:(t + 1) * LANES]
            end_ref[piece, depth:depth + PIECE_PAD] = decay[:, t * LANES:(t + 1) * LANES]


def gate_ssd_kernel(dims, sp_size, end_ref, own_ref, oth_ref, wt_ref, act_ref, dts_ref, oh_ref, ds_ref, z_ref, y_ref, in_ref,
                    x_buf, weights, state, gathered, starts, received, xsems, wsems, send_sem, recv_sem, send_sem2, recv_sem2):
    n_groups, group_inner, n_state, head_rep, half = dims
    conv_cols = group_inner + 2 * n_state
    group_cols = 2 * group_inner + 2 * n_state + head_rep
    n_heads = n_groups * head_rep
    depth = starts.shape[1]
    step_id = pl.program_id(0)
    n_z = 2 * n_groups
    me = lax.axis_index("sp")
    others = pl.ds(0, sp_size - 1)
    sent = pl.ds(0, depth + 1)
    mesh_id = pl.DeviceIdType.MESH

    def x_copy(k):
        return pltpu.make_async_copy((own_ref, oth_ref)[k], x_buf.at[k], xsems.at[k])

    @pl.when(step_id == 0)
    def _():
        weight_copy(wt_ref, weights, wsems, 0, group_cols, 0).start()
        x_copy(0).start()
        x_copy(1).start()
        barrier = pltpu.get_barrier_semaphore()

        def greet(k, carry):
            pl.semaphore_signal(barrier, inc=1, device_id={"sp": lax.rem(me + k, sp_size)}, device_id_type=mesh_id)
            return carry

        lax.fori_loop(1, sp_size, greet, 0)

    @pl.when(step_id == 1)
    def _():
        pl.semaphore_wait(pltpu.get_barrier_semaphore(), sp_size - 1)

        def send_out(k, carry):
            peer = lax.rem(me + k, sp_size)
            pltpu.make_async_remote_copy(
                src_ref=end_ref.at[peer, sent], dst_ref=gathered.at[me, sent], send_sem=send_sem, recv_sem=recv_sem,
                device_id={"sp": peer}, device_id_type=mesh_id).start()
            return carry

        lax.fori_loop(1, sp_size, send_out, 0)

    @pl.when(step_id == n_z)
    def _():
        state[...] = jnp.zeros_like(state)

    @pl.when(step_id == n_z + 2)
    def _():
        pltpu.make_async_copy(end_ref.at[others, sent], gathered.at[others, sent], recv_sem).wait()
        pltpu.make_async_copy(end_ref.at[others, sent], gathered.at[others, sent], send_sem).wait()
        gathered[me] = end_ref[me]

        def scan_step(j, carry):
            starts[j] = carry
            return gathered[j, depth:depth + 1] * carry + gathered[j, 0:depth]

        lax.fori_loop(0, sp_size, scan_step, jnp.zeros((depth, LANES), F32), unroll=4)

        def send_back(k, carry):
            peer = lax.rem(me + k, sp_size)
            pltpu.make_async_remote_copy(
                src_ref=starts.at[peer], dst_ref=received.at[me], send_sem=send_sem2, recv_sem=recv_sem2,
                device_id={"sp": peer}, device_id_type=mesh_id).start()
            return carry

        lax.fori_loop(1, sp_size, send_back, 0)

    @pl.when(step_id < n_z)
    def _():
        group_id, slot = step_id // 2, lax.rem(step_id, 2)

        @pl.when(slot == 0)
        def _():
            weight_copy(wt_ref, weights, wsems, group_id, group_cols, 0).wait()

        @pl.when((slot == 0) & (group_id < n_groups - 1))
        def _():
            weight_copy(wt_ref, weights, wsems, group_id + 1, group_cols, 0).start()

        for k in range(2):
            @pl.when(step_id == k)
            def _(k=k):
                x_copy(k).wait()

        z_ref[0] = lax.dot_general(x_buf[slot], weights[lax.rem(group_id, 2)], CONTRACT_LAST, preferred_element_type=F32).astype(BF16)

    @pl.when(step_id >= n_z)
    def _():
        dt_step = dts_ref[0]
        cum = dts_ref[1]
        seg_total = cum[SEG - 1:SEG]
        end_v = jnp.exp2(seg_total - cum) * dt_step
        start_v = jnp.exp2(cum)
        lane = lax.broadcasted_iota(jnp.int32, (SEG, LANES), 1)
        flipped = jnp.where(lane < n_heads, cum, dt_step).T
        row_id = lax.broadcasted_iota(jnp.int32, (SEG, SEG), 0)
        causal = row_id >= lane
        first_half = lane < LANES // 2

        for g in range(n_groups):
            c0 = g * conv_cols
            i0, i1 = g * group_inner, (g + 1) * group_inner
            x_mat = act_ref[:, c0:c0 + group_inner]
            end_w = spread(end_v, oh_ref[:, i0:i1])
            from_start = spread(start_v, oh_ref[:, i0:i1])
            b_mat = act_ref[:, c0 + group_inner:c0 + group_inner + n_state]
            c_mat = act_ref[:, c0 + group_inner + n_state:c0 + conv_cols]
            c_dot_b = lax.dot_general(c_mat, b_mat, (((1,), (1,)), ((), ())), preferred_element_type=F32)
            held = state[:, i0:i1]
            x_wide = x_mat.astype(F32)
            y_rest = jnp.dot(c_mat, held.astype(BF16), preferred_element_type=F32) * from_start + ds_ref[0:1, i0:i1] * x_wide
            for pair in range(head_rep // 2):
                scores = []
                for h in (g * head_rep + 2 * pair, g * head_rep + 2 * pair + 1):
                    gap = cum[:, h:h + 1] - flipped[h:h + 1]
                    weights = jnp.where(causal, jnp.exp2(gap), 0.0)
                    scores.append((c_dot_b * weights * flipped[n_heads + h:n_heads + h + 1]).astype(BF16))
                x_pair = x_mat[:, pair * LANES:(pair + 1) * LANES]
                zero = jnp.zeros_like(x_pair)
                x_both = jnp.concatenate([jnp.where(first_half, x_pair, zero), jnp.where(first_half, zero, x_pair)], axis=0)
                y_diag = jnp.dot(jnp.concatenate(scores, axis=1), x_both, preferred_element_type=F32)
                y_ref[:, i0 + pair * LANES:i0 + (pair + 1) * LANES] = y_rest[:, pair * LANES:(pair + 1) * LANES] + y_diag
            weighted = (x_wide * end_w).astype(BF16)
            new = lax.dot_general(b_mat, weighted, (((0,), (0,)), ((), ())), preferred_element_type=F32)
            state[:, i0:i1] = held * from_start[SEG - 1:SEG] + new

    @pl.when(step_id == pl.num_programs(0) - 1)
    def _():
        pltpu.make_async_copy(starts.at[others], received.at[others], recv_sem2).wait()
        pltpu.make_async_copy(starts.at[others], received.at[others], send_sem2).wait()
        received[me] = starts[me]
        in_ref[...] = received[...]


def gate_out_kernel(dims, y_ref, c0_ref, c1_ref, c2_ref, c3_ref, z_ref, dts_ref, in_ref, oh_ref, nw_ref, wo_hbm, tok_ref, out_ref,
                    wo_ref, state, o_next, o_prev, parts, received, wsem, send_sems, recv_sems):
    n_groups, group_inner, n_state, head_rep, half = dims
    step_id = pl.program_id(0)
    n_tiles = half // SUB
    peer = {"tp": 1 - lax.axis_index("tp")} if EXCHANGE else None

    def send(k):
        return pltpu.make_async_remote_copy(
            src_ref=parts.at[k], dst_ref=received.at[k], send_sem=send_sems.at[k], recv_sem=recv_sems.at[k],
            device_id=peer, device_id_type=pl.DeviceIdType.MESH)

    def gate_rows():
        from_start = spread(jnp.exp2(dts_ref[0]), oh_ref[...])
        for g, c_ref in enumerate((c0_ref, c1_ref, c2_ref, c3_ref)):
            i0, i1 = g * group_inner, (g + 1) * group_inner
            y_in = jnp.dot(c_ref[...], state[:, i0:i1], preferred_element_type=F32)
            y_ssd = y_ref[:, i0:i1] + y_in * from_start[:, i0:i1]
            gate = z_ref[0, :, i0:i1].astype(F32)
            gated = y_ssd * (gate / (1.0 + jnp.exp(-gate)))
            inv_rms = lax.rsqrt(jnp.mean(gated * gated, axis=-1, keepdims=True) + NORM_EPS)
            o_next[:, i0:i1] = (gated * inv_rms * nw_ref[0:1, i0:i1].astype(F32)).astype(BF16)

    def out_rows():
        parts[jnp.minimum(step_id - 1, n_tiles)] = jnp.dot(o_prev[...], wo_ref[...], preferred_element_type=F32).astype(BF16)

    wo_copy = pltpu.make_async_copy(wo_hbm, wo_ref, wsem)

    @pl.when(step_id == 0)
    def _():
        wo_copy.start()
        if EXCHANGE:
            pl.semaphore_signal(pltpu.get_barrier_semaphore(), inc=1, device_id=peer, device_id_type=pl.DeviceIdType.MESH)
        lane_tiles = n_groups * group_inner // LANES
        quarters = in_ref.shape[0] // lane_tiles
        depth = n_state // quarters
        for t in range(lane_tiles):
            for q in range(quarters):
                state[q * depth:(q + 1) * depth, t * LANES:(t + 1) * LANES] = in_ref[t * quarters + q].astype(BF16)
        gate_rows()
        wo_copy.wait()
        if EXCHANGE:
            pl.semaphore_wait(pltpu.get_barrier_semaphore(), 1)

    @pl.when((step_id > 0) & (step_id < 2 * n_tiles))
    def _():
        out_rows()
        gate_rows()

    @pl.when(step_id == 2 * n_tiles)
    def _():
        out_rows()

    o_prev[...] = o_next[...]

    if EXCHANGE:
        for k in range(n_tiles):
            @pl.when(step_id == k + 1)
            def _(k=k):
                send(k).start()

            @pl.when(step_id == n_tiles + 1 + k)
            def _(k=k):
                send(k).wait_recv()

    @pl.when(step_id > n_tiles)
    def _():
        got = received[jnp.maximum(step_id - n_tiles - 1, 0)]
        out_ref[...] = (tok_ref[...].astype(F32) + parts[n_tiles].astype(F32) + got.astype(F32)).astype(BF16)

    if EXCHANGE:
        @pl.when(step_id == 2 * n_tiles)
        def _():
            for k in range(n_tiles):
                send(k).wait_send()


def solution(mesh):
    sp_size, tp_size = mesh.shape["sp"], mesh.shape["tp"]
    row_spec = P(("dp", "sp", "tp"), None)
    swap = [(0, 1), (1, 0)]

    def layer_block(tokens, w_in, conv_w, conv_bias, a_log, dt_bias, d_skip, norm_w, w_out):
        n_groups, conv_cols = conv_bias.shape
        n_heads = a_log.shape[0]
        inner_dim = norm_w.shape[0]
        head_rep = n_heads // n_groups
        group_inner = inner_dim // n_groups
        head_dim = inner_dim // n_heads
        n_state = (conv_cols - group_inner) // 2
        half, width = tokens.shape
        rows = 2 * half
        all_conv = n_groups * conv_cols
        dims = (n_groups, group_inner, n_state, head_rep, half)
        tp_idx = lax.axis_index("tp")
        tp_arr = tp_idx.reshape(1).astype(jnp.int32)
        any_spec = pl.BlockSpec(memory_space=pl.ANY)
        limit = 60 * 2**20
        w_in_t = w_in.T

        other = lax.ppermute(tokens, "tp", swap)
        tail = tokens[half - HALO:]
        edge = [(2 * i + 1, 2 * i + 2) for i in range(sp_size - 1)]
        edge_same = [(2 * i + 1, 2 * i + 3) for i in range(sp_size - 1)]
        halo = lax.ppermute(tail, ("sp", "tp"), edge) + lax.ppermute(tail, ("sp", "tp"), edge_same)

        head_par = jnp.concatenate([jnp.tile(a_log, 4)[None], jnp.tile(dt_bias, 4)[None]], axis=0)
        skip_row = jnp.repeat(d_skip, head_dim)[None]
        head_of = jnp.arange(inner_dim) // head_dim
        lane_head = jnp.where(jnp.arange(LANES) < 3 * n_heads, jnp.arange(LANES) % n_heads, -1)
        one_hot = (lane_head[:, None] == head_of[None, :]).astype(BF16)
        cw = conv_w.reshape(4, all_conv).astype(F32)
        cb = conv_bias.reshape(1, all_conv).astype(F32)

        n_pieces = sp_size
        depth = n_state * inner_dim // LANES // n_pieces
        once = dict(pipeline_mode=pl.Buffered(buffer_count=1))
        act, dts, end_state = pl.pallas_call(
            functools.partial(project_conv_kernel, dims),
            grid_spec=pltpu.PrefetchScalarGridSpec(
                num_scalar_prefetch=1, grid=(n_groups,),
                in_specs=[
                    any_spec, any_spec, any_spec, any_spec,
                    pl.BlockSpec((4, conv_cols), lambda g, tp: (0, g)),
                    pl.BlockSpec((1, conv_cols), lambda g, tp: (0, g)),
                    pl.BlockSpec((2, LANES), lambda g, tp: (0, 0)),
                    pl.BlockSpec((LANES, group_inner), lambda g, tp: (0, g)),
                ],
                out_specs=[
                    pl.BlockSpec((rows, conv_cols), lambda g, tp: (0, g)),
                    pl.BlockSpec((3, rows, LANES), lambda g, tp: (0, 0, 0), **once),
                    pl.BlockSpec((n_pieces, depth + PIECE_PAD, LANES), lambda g, tp: (0, 0, 0), **once),
                ],
                scratch_shapes=[
                    pltpu.VMEM((2, HALO + half, width), BF16),
                    pltpu.VMEM((2, conv_cols, width), BF16),
                    pltpu.VMEM((LANES, width), BF16),
                    pltpu.VMEM((conv_cols // LANES, HALO + SUB, LANES), F32),
                    pltpu.VMEM((conv_cols // LANES, HALO + SUB, LANES), F32),
                    pltpu.VMEM((conv_cols // LANES, HALO + SUB, LANES), F32),
                    pltpu.VMEM((conv_cols // LANES, HALO + SUB, LANES), F32),
                    pltpu.VMEM((n_state, group_inner), F32),
                    pltpu.VMEM((1, LANES), F32),
                    pltpu.SemaphoreType.DMA((4,)),
                    pltpu.SemaphoreType.DMA((2,)),
                    pltpu.SemaphoreType.DMA((n_groups,)),
                ]),
            out_shape=[
                jax.ShapeDtypeStruct((rows, all_conv), BF16),
                jax.ShapeDtypeStruct((3, rows, LANES), F32),
                jax.ShapeDtypeStruct((n_pieces, depth + PIECE_PAD, LANES), F32),
            ],
            compiler_params=pltpu.CompilerParams(vmem_limit_bytes=limit),
            cost_estimate=pl.CostEstimate(flops=2 * rows * width * all_conv, bytes_accessed=2 * width * all_conv, transcendentals=0),
            name="project_conv_states",
        )(tp_arr, tokens, other, halo, w_in_t, cw, cb, head_par, one_hot)

        n_z = 2 * n_groups

        def seg_at(i):
            return jnp.maximum(i - n_z, 0)

        def z_at(i):
            return jnp.minimum(i, n_z - 1)

        gate_z, y_local, incoming = pl.pallas_call(
            functools.partial(gate_ssd_kernel, dims, sp_size),
            grid=(n_z + rows // SEG,),
            in_specs=[
                pl.BlockSpec((n_pieces, depth + PIECE_PAD, LANES), lambda i: (0, 0, 0), **once),
                any_spec, any_spec, any_spec,
                pl.BlockSpec((SEG, all_conv), lambda i: (seg_at(i), 0)),
                pl.BlockSpec((2, SEG, LANES), lambda i: (0, seg_at(i), 0)),
                pl.BlockSpec((LANES, inner_dim), lambda i: (0, 0), **once),
                pl.BlockSpec((1, inner_dim), lambda i: (0, 0)),
            ],
            out_specs=[
                pl.BlockSpec((1, half, group_inner), lambda i: (lax.rem(z_at(i), 2), 0, z_at(i) // 2)),
                pl.BlockSpec((SEG, inner_dim), lambda i: (seg_at(i), 0)),
                pl.BlockSpec((n_pieces, depth, LANES), lambda i: (0, 0, 0), **once),
            ],
            out_shape=[
                jax.ShapeDtypeStruct((2, half, inner_dim), BF16),
                jax.ShapeDtypeStruct((rows, inner_dim), F32),
                jax.ShapeDtypeStruct((n_pieces, depth, LANES), F32),
            ],
            scratch_shapes=[
                pltpu.VMEM((2, half, width), BF16),
                pltpu.VMEM((2, group_inner, width), BF16),
                pltpu.VMEM((n_state, inner_dim), F32),
                pltpu.VMEM((n_pieces, depth + PIECE_PAD, LANES), F32),
                pltpu.VMEM((n_pieces, depth, LANES), F32),
                pltpu.VMEM((n_pieces, depth, LANES), F32),
                pltpu.SemaphoreType.DMA((2,)),
                pltpu.SemaphoreType.DMA((2,)),
                pltpu.SemaphoreType.DMA, pltpu.SemaphoreType.DMA,
                pltpu.SemaphoreType.DMA, pltpu.SemaphoreType.DMA,
            ],
            compiler_params=pltpu.CompilerParams(vmem_limit_bytes=limit, collective_id=0, has_side_effects=True),
            name="gate_ssd_exchange",
        )(end_state, tokens, other, w_in_t, act, dts, one_hot, skip_row)

        n_tiles = half // SUB

        def tile(i):
            return jnp.minimum(i, 2 * n_tiles - 1)

        def slot_of(i):
            return 1 - tile(i) // n_tiles

        def row_at(i):
            return lax.rem(lax.axis_index("tp") + slot_of(i), 2) * n_tiles + lax.rem(tile(i), n_tiles)

        def own_at(i):
            return jnp.maximum(i - n_tiles - 1, 0)

        def c_spec(g):
            return pl.BlockSpec((SUB, LANES), lambda i: (row_at(i), 6 * g + 5))

        return pl.pallas_call(
            functools.partial(gate_out_kernel, dims),
            grid=(2 * n_tiles + 1,),
            in_specs=[
                pl.BlockSpec((SUB, inner_dim), lambda i: (row_at(i), 0)),
                c_spec(0), c_spec(1), c_spec(2), c_spec(3),
                pl.BlockSpec((1, SUB, inner_dim), lambda i: (slot_of(i), lax.rem(tile(i), n_tiles), 0)),
                pl.BlockSpec((1, SUB, LANES), lambda i: (2, row_at(i), 0)),
                pl.BlockSpec((n_pieces, depth, LANES), lambda i: (0, 0, 0), **once),
                pl.BlockSpec((LANES, inner_dim), lambda i: (0, 0), **once),
                pl.BlockSpec((1, inner_dim), lambda i: (0, 0)),
                any_spec,
                pl.BlockSpec((SUB, width), lambda i: (own_at(i), 0)),
            ],
            out_specs=pl.BlockSpec((SUB, width), lambda i: (own_at(i), 0)),
            out_shape=jax.ShapeDtypeStruct((half, width), BF16),
            scratch_shapes=[
                pltpu.VMEM((inner_dim, width), BF16),
                pltpu.VMEM((n_state, inner_dim), BF16),
                pltpu.VMEM((SUB, inner_dim), BF16),
                pltpu.VMEM((SUB, inner_dim), BF16),
                pltpu.VMEM((n_tiles + 1, SUB, width), BF16),
                pltpu.VMEM((n_tiles, SUB, width), BF16),
                pltpu.SemaphoreType.DMA,
                pltpu.SemaphoreType.DMA((n_tiles,)),
                pltpu.SemaphoreType.DMA((n_tiles,)),
            ],
            compiler_params=pltpu.CompilerParams(vmem_limit_bytes=limit, **(dict(collective_id=1, has_side_effects=True) if EXCHANGE else {})),
            name="gate_out_swap",
        )(y_local, act, act, act, act, gate_z, dts, incoming, one_hot, norm_w[None], w_out, tokens)

    return jax.shard_map(
        layer_block,
        mesh=mesh,
        in_specs=(row_spec, P(None, "tp"), P(None, "tp", None), P("tp", None), P("tp"), P("tp"), P("tp"), P("tp"), P("tp", None)),
        out_specs=row_spec,
        check_vma=False)
```

```python
import functools

import jax
import jax.numpy as jnp
import numpy as np
from jax import lax
from jax.experimental import pallas as pl
from jax.experimental.pallas import tpu as pltpu
from jax.sharding import PartitionSpec as P

SEG = 128
SUB = 256
HALO = 16
EXCHANGE = True
NORM_EPS = 1e-5
LANES = 128
PIECE_PAD = 8
LOG2E = 1.4426950408889634
F32 = jnp.float32
BF16 = jnp.bfloat16


def spread(values, one_hot):
    n_heads = LANES // 4
    high = values.astype(BF16)
    rest = values - high.astype(F32)
    mid = rest.astype(BF16)
    low = (rest - mid.astype(F32)).astype(BF16)
    lane = lax.broadcasted_iota(jnp.int32, values.shape, 1)
    parts = jnp.where(lane < n_heads, high.astype(F32), jnp.where(lane < 2 * n_heads, mid.astype(F32), low.astype(F32)))
    parts = jnp.where(lane < 3 * n_heads, parts, 0.0).astype(BF16)
    return jnp.dot(parts, one_hot, preferred_element_type=F32)


CONTRACT_LAST = (((1,), (1,)), ((), ()))


def weight_copy(wt_ref, weights, sems, group_id, group_cols, offset):
    rows = weights.shape[1]
    lo = pl.multiple_of(group_id * group_cols + offset, 8)
    slot = lax.rem(group_id, 2)
    return pltpu.make_async_copy(wt_ref.at[pl.ds(lo, rows)], weights.at[slot], sems.at[slot])


def project_conv_kernel(dims, tp_ref, own_ref, oth_ref, halo_ref, wt_ref,
                        cw_ref, cb_ref, al_ref, db_ref, oh_ref, act_ref, dts_ref, end_ref, held_ref,
                        x_buf, weights, w_dt, ext0, ext1, ext2, ext3, state, total, sems, wsems, dsems):
    n_groups, group_inner, n_state, head_rep, half = dims
    group_id = pl.program_id(0)
    n_heads = n_groups * head_rep
    exts = (ext0, ext1, ext2, ext3)

    def copies(first, second):
        return [
            lambda: pltpu.make_async_copy(halo_ref, x_buf.at[0, pl.ds(0, HALO)], sems.at[0]),
            lambda: pltpu.make_async_copy(first, x_buf.at[0, pl.ds(HALO, half)], sems.at[1]),
            lambda: pltpu.make_async_copy(first.at[pl.ds(half - HALO, HALO)], x_buf.at[1, pl.ds(0, HALO)], sems.at[2]),
            lambda: pltpu.make_async_copy(second, x_buf.at[1, pl.ds(HALO, half)], sems.at[3]),
        ]

    start = group_id == 0

    @pl.when(start & (tp_ref[0] == 0))
    def _():
        for c in copies(own_ref, oth_ref):
            c().start()

    @pl.when(start & (tp_ref[0] == 1))
    def _():
        for c in copies(oth_ref, own_ref):
            c().start()

    group_cols = 2 * group_inner + 2 * n_state + head_rep
    dt_copies = [
        pltpu.make_async_copy(wt_ref.at[pl.ds((g + 1) * group_cols - head_rep, head_rep)], w_dt.at[pl.ds(g * head_rep, head_rep)], dsems.at[g])
        for g in range(n_groups)]

    @pl.when(start)
    def _():
        weight_copy(wt_ref, weights, wsems, group_id, group_cols, group_inner).start()
        w_dt[n_heads:LANES] = jnp.zeros((LANES - n_heads, w_dt.shape[1]), BF16)
        for c in dt_copies:
            c.start()
        total[...] = jnp.zeros_like(total)
        for c in dt_copies:
            c.wait()
        for c in copies(own_ref, oth_ref)[:2]:
            c().wait()

    weight_copy(wt_ref, weights, wsems, group_id, group_cols, group_inner).wait()
    state[...] = jnp.zeros_like(state)

    @pl.when(group_id < n_groups - 1)
    def _():
        weight_copy(wt_ref, weights, wsems, group_id + 1, group_cols, group_inner).start()

    w_slot = lax.rem(group_id, 2)

    def steps_of(half_id):
        def step(s, carry):
            at = pl.ds(pl.multiple_of(HALO + s * SUB, 16), SUB)
            raw = lax.dot_general(x_buf[half_id, at, :], w_dt[...], CONTRACT_LAST, preferred_element_type=F32).astype(BF16).astype(F32)
            raw = raw + pltpu.roll(raw, n_heads, 1) + pltpu.roll(raw, 2 * n_heads, 1) + pltpu.roll(raw, 3 * n_heads, 1)
            dt_step = jax.nn.softplus(raw + jnp.concatenate([db_ref[...]] * 4, axis=1))
            log_decay = -jnp.exp(jnp.concatenate([al_ref[...]] * 4, axis=1)) * dt_step * LOG2E
            row_id = lax.broadcasted_iota(jnp.int32, (SEG, SEG), 0)
            col_id = lax.broadcasted_iota(jnp.int32, (SEG, SEG), 1)
            tri = (row_id >= col_id).astype(F32)
            for q in range(SUB // SEG):
                lo, hi = q * SEG, (q + 1) * SEG
                cum = jnp.dot(tri, log_decay[lo:hi], precision=lax.Precision.HIGHEST, preferred_element_type=F32)
                out = pl.ds(pl.multiple_of(half_id * half + s * SUB + lo, SEG), SEG)
                dts_ref[0, out, :] = dt_step[lo:hi]
                dts_ref[1, out, :] = cum
                dts_ref[2, out, :] = cum + total[...]
                total[...] += cum[SEG - 1:SEG]
            return carry
        lax.fori_loop(0, half // SUB, step, 0)

    @pl.when(group_id == 0)
    def _():
        steps_of(0)

    n_cols = weights.shape[1] // LANES

    def matmul(half_id, s):
        lo = 0 if s == 0 else HALO
        rows = x_buf[half_id, s * SUB + lo:HALO + (s + 1) * SUB, :]
        raw = lax.dot_general(rows, weights[w_slot], CONTRACT_LAST, preferred_element_type=F32).astype(BF16).astype(F32)
        for t in range(n_cols):
            exts[s][t, lo:HALO + SUB] = raw[:, t * LANES:(t + 1) * LANES]

    def convolved(half_id, s, t):
        ext = exts[s]
        if s > 0:
            ext[t, 8:HALO] = exts[s - 1][t, HALO + SUB - 8:HALO + SUB]
        lanes = slice(t * LANES, (t + 1) * LANES)
        acc = cb_ref[:, lanes] + ext[t, HALO - 3:HALO - 3 + SUB] * cw_ref[0:1, lanes]
        for k in range(1, 4):
            acc = acc + ext[t, HALO - 3 + k:HALO - 3 + k + SUB] * cw_ref[k:k + 1, lanes]
        act = (acc / (1.0 + jnp.exp(-acc))).astype(BF16)
        act_ref[half_id * half + s * SUB:half_id * half + (s + 1) * SUB, lanes] = act
        return act

    def vector(half_id, s):
        n_x = group_inner // LANES
        b_all = convolved(half_id, s, n_x)
        convolved(half_id, s, n_x + 1)
        at = slice(half_id * half + s * SUB, half_id * half + (s + 1) * SUB)
        dt_step, cum = dts_ref[0, at, :], dts_ref[1, at, :]
        ends = [cum[(q + 1) * SEG - 1:(q + 1) * SEG] for q in range(SUB // SEG)]
        last = jnp.concatenate([jnp.broadcast_to(e, (SEG, LANES)) for e in ends], axis=0)
        end_w = spread(jnp.exp2(last - cum) * dt_step, oh_ref[...])
        decay = spread(jnp.exp2(jnp.concatenate([jnp.broadcast_to(e, (8, LANES)) for e in ends], axis=0)), oh_ref[...])
        weighted = [(convolved(half_id, s, t).astype(F32) * end_w[:, t * LANES:(t + 1) * LANES]).astype(BF16) for t in range(n_x)]
        weighted = jnp.concatenate(weighted, axis=1)
        for q in range(SUB // SEG):
            lo, hi = q * SEG, (q + 1) * SEG
            new = lax.dot_general(b_all[lo:hi], weighted[lo:hi], (((0,), (0,)), ((), ())), preferred_element_type=F32)
            before = state[...]
            held_ref[(half_id * half + s * SUB) // SEG + q] = before.astype(BF16)
            state[...] = before * decay[8 * q:8 * q + 1] + new

    order = [(h, s) for h in range(2) for s in range(half // SUB)]
    matmul(*order[0])
    for k in range(1, len(order)):
        if order[k] == (1, 0):
            @pl.when(group_id == 0)
            def _():
                for c in copies(own_ref, oth_ref)[2:]:
                    c().wait()
                steps_of(1)
        matmul(*order[k])
        vector(*order[k - 1])
    vector(*order[-1])

    decay = spread(jnp.exp2(jnp.broadcast_to(total[...], (8, LANES))), oh_ref[...])
    n_tiles = group_inner // LANES
    quarters = end_ref.shape[0] // (n_groups * n_tiles)
    depth = n_state // quarters
    for t in range(n_tiles):
        for q in range(quarters):
            piece = (group_id * n_tiles + t) * quarters + q
            end_ref[piece, 0:depth] = state[q * depth:(q + 1) * depth, t * LANES:(t + 1) * LANES]
            end_ref[piece, depth:depth + PIECE_PAD] = decay[:, t * LANES:(t + 1) * LANES]


def gate_ssd_kernel(dims, sp_size, end_ref, own_ref, oth_ref, wt_ref, act_ref, dts_ref, held_ref, oh_ref, ds_ref, z_ref, y_ref, in_ref,
                    x_buf, weights, gathered, starts, received, xsems, wsems, send_sem, recv_sem, send_sem2, recv_sem2):
    n_groups, group_inner, n_state, head_rep, half = dims
    conv_cols = group_inner + 2 * n_state
    group_cols = 2 * group_inner + 2 * n_state + head_rep
    n_heads = n_groups * head_rep
    depth = starts.shape[1]
    step_id = pl.program_id(0)
    n_z = 2 * n_groups
    me = lax.axis_index("sp")
    others = pl.ds(0, sp_size - 1)
    sent = pl.ds(0, depth + 1)
    mesh_id = pl.DeviceIdType.MESH

    def x_copy(k):
        return pltpu.make_async_copy((own_ref, oth_ref)[k], x_buf.at[k], xsems.at[k])

    @pl.when(step_id == 0)
    def _():
        weight_copy(wt_ref, weights, wsems, 0, group_cols, 0).start()
        x_copy(0).start()
        x_copy(1).start()
        barrier = pltpu.get_barrier_semaphore()

        def greet(k, carry):
            pl.semaphore_signal(barrier, inc=1, device_id={"sp": lax.rem(me + k, sp_size)}, device_id_type=mesh_id)
            return carry

        lax.fori_loop(1, sp_size, greet, 0)

    @pl.when(step_id == 1)
    def _():
        pl.semaphore_wait(pltpu.get_barrier_semaphore(), sp_size - 1)

        def send_out(k, carry):
            peer = lax.rem(me + k, sp_size)
            pltpu.make_async_remote_copy(
                src_ref=end_ref.at[peer, sent], dst_ref=gathered.at[me, sent], send_sem=send_sem, recv_sem=recv_sem,
                device_id={"sp": peer}, device_id_type=mesh_id).start()
            return carry

        lax.fori_loop(1, sp_size, send_out, 0)

    @pl.when(step_id == n_z + 1)
    def _():
        pltpu.make_async_copy(end_ref.at[others, sent], gathered.at[others, sent], recv_sem).wait()
        pltpu.make_async_copy(end_ref.at[others, sent], gathered.at[others, sent], send_sem).wait()
        gathered[me] = end_ref[me]

        def scan_step(j, carry):
            starts[j] = carry
            return gathered[j, depth:depth + 1] * carry + gathered[j, 0:depth]

        lax.fori_loop(0, sp_size, scan_step, jnp.zeros((depth, LANES), F32), unroll=4)

        def send_back(k, carry):
            peer = lax.rem(me + k, sp_size)
            pltpu.make_async_remote_copy(
                src_ref=starts.at[peer], dst_ref=received.at[me], send_sem=send_sem2, recv_sem=recv_sem2,
                device_id={"sp": peer}, device_id_type=mesh_id).start()
            return carry

        lax.fori_loop(1, sp_size, send_back, 0)

    @pl.when(step_id < n_z)
    def _():
        group_id, slot = step_id // 2, lax.rem(step_id, 2)

        @pl.when(slot == 0)
        def _():
            weight_copy(wt_ref, weights, wsems, group_id, group_cols, 0).wait()

        @pl.when((slot == 0) & (group_id < n_groups - 1))
        def _():
            weight_copy(wt_ref, weights, wsems, group_id + 1, group_cols, 0).start()

        for k in range(2):
            @pl.when(step_id == k)
            def _(k=k):
                x_copy(k).wait()

        z_ref[0] = lax.dot_general(x_buf[slot], weights[lax.rem(group_id, 2)], CONTRACT_LAST, preferred_element_type=F32).astype(BF16)

    def segment(q):
        at = slice(q * SEG, (q + 1) * SEG)
        dt_step = dts_ref[0, at]
        cum = dts_ref[1, at]
        start_v = jnp.exp2(cum)
        lane = lax.broadcasted_iota(jnp.int32, (SEG, LANES), 1)
        flipped = jnp.where(lane < n_heads, cum, dt_step).T
        row_id = lax.broadcasted_iota(jnp.int32, (SEG, SEG), 0)
        causal = row_id >= lane
        first_half = lane < LANES // 2

        for g in range(n_groups):
            c0 = g * conv_cols
            i0, i1 = g * group_inner, (g + 1) * group_inner
            x_mat = act_ref[at, c0:c0 + group_inner]
            from_start = spread(start_v, oh_ref[:, i0:i1])
            b_mat = act_ref[at, c0 + group_inner:c0 + group_inner + n_state]
            c_mat = act_ref[at, c0 + group_inner + n_state:c0 + conv_cols]
            c_dot_b = lax.dot_general(c_mat, b_mat, (((1,), (1,)), ((), ())), preferred_element_type=F32)
            x_wide = x_mat.astype(F32)
            y_rest = jnp.dot(c_mat, held_ref[q, :, i0:i1], preferred_element_type=F32) * from_start + ds_ref[0:1, i0:i1] * x_wide
            for pair in range(head_rep // 2):
                scores = []
                for h in (g * head_rep + 2 * pair, g * head_rep + 2 * pair + 1):
                    gap = cum[:, h:h + 1] - flipped[h:h + 1]
                    weights = jnp.where(causal, jnp.exp2(gap), 0.0)
                    scores.append((c_dot_b * weights * flipped[n_heads + h:n_heads + h + 1]).astype(BF16))
                x_pair = x_mat[:, pair * LANES:(pair + 1) * LANES]
                zero = jnp.zeros_like(x_pair)
                x_both = jnp.concatenate([jnp.where(first_half, x_pair, zero), jnp.where(first_half, zero, x_pair)], axis=0)
                y_diag = jnp.dot(jnp.concatenate(scores, axis=1), x_both, preferred_element_type=F32)
                y_ref[at, i0 + pair * LANES:i0 + (pair + 1) * LANES] = y_rest[:, pair * LANES:(pair + 1) * LANES] + y_diag

    @pl.when(step_id >= n_z)
    def _():
        for q in range(SUB // SEG):
            segment(q)

    @pl.when(step_id == pl.num_programs(0) - 1)
    def _():
        pltpu.make_async_copy(starts.at[others], received.at[others], recv_sem2).wait()
        pltpu.make_async_copy(starts.at[others], received.at[others], send_sem2).wait()
        received[me] = starts[me]
        in_ref[...] = received[...]


def gate_out_kernel(dims, y_ref, c0_ref, c1_ref, c2_ref, c3_ref, z_ref, dts_ref, in_ref, oh_ref, nw_ref, wo_hbm, tok_ref, out_ref,
                    wo_ref, state, o_next, o_prev, parts, received, wsem, send_sems, recv_sems):
    n_groups, group_inner, n_state, head_rep, half = dims
    step_id = pl.program_id(0)
    n_tiles = half // SUB
    peer = {"tp": 1 - lax.axis_index("tp")} if EXCHANGE else None

    def send(k):
        return pltpu.make_async_remote_copy(
            src_ref=parts.at[k], dst_ref=received.at[k], send_sem=send_sems.at[k], recv_sem=recv_sems.at[k],
            device_id=peer, device_id_type=pl.DeviceIdType.MESH)

    def gate_rows():
        from_start = spread(jnp.exp2(dts_ref[0]), oh_ref[...])
        for g, c_ref in enumerate((c0_ref, c1_ref, c2_ref, c3_ref)):
            i0, i1 = g * group_inner, (g + 1) * group_inner
            y_in = jnp.dot(c_ref[...], state[:, i0:i1], preferred_element_type=F32)
            y_ssd = y_ref[:, i0:i1] + y_in * from_start[:, i0:i1]
            gate = z_ref[0, :, i0:i1].astype(F32)
            gated = y_ssd * (gate / (1.0 + jnp.exp(-gate)))
            inv_rms = lax.rsqrt(jnp.mean(gated * gated, axis=-1, keepdims=True) + NORM_EPS)
            o_next[:, i0:i1] = (gated * inv_rms * nw_ref[0:1, i0:i1].astype(F32)).astype(BF16)

    def out_rows():
        parts[jnp.minimum(step_id - 1, n_tiles)] = jnp.dot(o_prev[...], wo_ref[...], preferred_element_type=F32).astype(BF16)

    wo_copy = pltpu.make_async_copy(wo_hbm, wo_ref, wsem)

    @pl.when(step_id == 0)
    def _():
        wo_copy.start()
        if EXCHANGE:
            pl.semaphore_signal(pltpu.get_barrier_semaphore(), inc=1, device_id=peer, device_id_type=pl.DeviceIdType.MESH)
        lane_tiles = n_groups * group_inner // LANES
        quarters = in_ref.shape[0] // lane_tiles
        depth = n_state // quarters
        for t in range(lane_tiles):
            for q in range(quarters):
                state[q * depth:(q + 1) * depth, t * LANES:(t + 1) * LANES] = in_ref[t * quarters + q].astype(BF16)
        gate_rows()
        wo_copy.wait()
        if EXCHANGE:
            pl.semaphore_wait(pltpu.get_barrier_semaphore(), 1)

    @pl.when((step_id > 0) & (step_id < 2 * n_tiles))
    def _():
        out_rows()
        gate_rows()

    @pl.when(step_id == 2 * n_tiles)
    def _():
        out_rows()

    o_prev[...] = o_next[...]

    if EXCHANGE:
        for k in range(n_tiles):
            @pl.when(step_id == k + 1)
            def _(k=k):
                send(k).start()

            @pl.when(step_id == n_tiles + 1 + k)
            def _(k=k):
                send(k).wait_recv()

    @pl.when(step_id > n_tiles)
    def _():
        got = received[jnp.maximum(step_id - n_tiles - 1, 0)]
        out_ref[...] = (tok_ref[...].astype(F32) + parts[n_tiles].astype(F32) + got.astype(F32)).astype(BF16)

    if EXCHANGE:
        @pl.when(step_id == 2 * n_tiles)
        def _():
            for k in range(n_tiles):
                send(k).wait_send()


def solution(mesh):
    sp_size, tp_size = mesh.shape["sp"], mesh.shape["tp"]
    row_spec = P(("dp", "sp", "tp"), None)
    swap = [(0, 1), (1, 0)]

    def layer_block(tokens, w_in, conv_w, conv_bias, a_log, dt_bias, d_skip, norm_w, w_out):
        n_groups, conv_cols = conv_bias.shape
        n_heads = a_log.shape[0]
        inner_dim = norm_w.shape[0]
        head_rep = n_heads // n_groups
        group_inner = inner_dim // n_groups
        head_dim = inner_dim // n_heads
        n_state = (conv_cols - group_inner) // 2
        half, width = tokens.shape
        rows = 2 * half
        all_conv = n_groups * conv_cols
        dims = (n_groups, group_inner, n_state, head_rep, half)
        tp_idx = lax.axis_index("tp")
        tp_arr = tp_idx.reshape(1).astype(jnp.int32)
        any_spec = pl.BlockSpec(memory_space=pl.ANY)
        limit = 60 * 2**20
        w_in_t = w_in.T

        other = lax.ppermute(tokens, "tp", swap)
        tail = tokens[half - HALO:]
        edge = [(2 * i + 1, 2 * i + 2) for i in range(sp_size - 1)]
        edge_same = [(2 * i + 1, 2 * i + 3) for i in range(sp_size - 1)]
        halo = lax.ppermute(tail, ("sp", "tp"), edge) + lax.ppermute(tail, ("sp", "tp"), edge_same)

        skip_row = jnp.repeat(d_skip, head_dim)[None]
        head_of = np.arange(inner_dim) // head_dim
        lane_head = np.where(np.arange(LANES) < 3 * n_heads, np.arange(LANES) % n_heads, -1)
        one_hot = jnp.asarray(lane_head[:, None] == head_of[None, :], BF16)
        cw = conv_w.reshape(4, all_conv).astype(F32)
        cb = conv_bias.reshape(1, all_conv).astype(F32)

        n_pieces = sp_size
        depth = n_state * inner_dim // LANES // n_pieces
        once = dict(pipeline_mode=pl.Buffered(buffer_count=1))
        act, dts, end_state, held = pl.pallas_call(
            functools.partial(project_conv_kernel, dims),
            grid_spec=pltpu.PrefetchScalarGridSpec(
                num_scalar_prefetch=1, grid=(n_groups,),
                in_specs=[
                    any_spec, any_spec, any_spec, any_spec,
                    pl.BlockSpec((4, conv_cols), lambda g, tp: (0, g)),
                    pl.BlockSpec((1, conv_cols), lambda g, tp: (0, g)),
                    pl.BlockSpec((1, n_heads), lambda g, tp: (0, 0)),
                    pl.BlockSpec((1, n_heads), lambda g, tp: (0, 0)),
                    pl.BlockSpec((LANES, group_inner), lambda g, tp: (0, g)),
                ],
                out_specs=[
                    pl.BlockSpec((rows, conv_cols), lambda g, tp: (0, g)),
                    pl.BlockSpec((3, rows, LANES), lambda g, tp: (0, 0, 0), **once),
                    pl.BlockSpec((n_pieces, depth + PIECE_PAD, LANES), lambda g, tp: (0, 0, 0), **once),
                    pl.BlockSpec((rows // SEG, n_state, group_inner), lambda g, tp: (0, 0, g)),
                ],
                scratch_shapes=[
                    pltpu.VMEM((2, HALO + half, width), BF16),
                    pltpu.VMEM((2, conv_cols, width), BF16),
                    pltpu.VMEM((LANES, width), BF16),
                    pltpu.VMEM((conv_cols // LANES, HALO + SUB, LANES), F32),
                    pltpu.VMEM((conv_cols // LANES, HALO + SUB, LANES), F32),
                    pltpu.VMEM((conv_cols // LANES, HALO + SUB, LANES), F32),
                    pltpu.VMEM((conv_cols // LANES, HALO + SUB, LANES), F32),
                    pltpu.VMEM((n_state, group_inner), F32),
                    pltpu.VMEM((1, LANES), F32),
                    pltpu.SemaphoreType.DMA((4,)),
                    pltpu.SemaphoreType.DMA((2,)),
                    pltpu.SemaphoreType.DMA((n_groups,)),
                ]),
            out_shape=[
                jax.ShapeDtypeStruct((rows, all_conv), BF16),
                jax.ShapeDtypeStruct((3, rows, LANES), F32),
                jax.ShapeDtypeStruct((n_pieces, depth + PIECE_PAD, LANES), F32),
                jax.ShapeDtypeStruct((rows // SEG, n_state, inner_dim), BF16),
            ],
            compiler_params=pltpu.CompilerParams(vmem_limit_bytes=limit),
            cost_estimate=pl.CostEstimate(flops=2 * rows * width * all_conv, bytes_accessed=2 * width * all_conv, transcendentals=0),
            name="project_conv_states",
        )(tp_arr, tokens, other, halo, w_in_t, cw, cb, a_log[None], dt_bias[None], one_hot)

        n_z = 2 * n_groups

        def seg_at(i):
            return jnp.maximum(i - n_z, 0)

        def z_at(i):
            return jnp.minimum(i, n_z - 1)

        gate_z, y_local, incoming = pl.pallas_call(
            functools.partial(gate_ssd_kernel, dims, sp_size),
            grid=(n_z + rows // SUB,),
            in_specs=[
                pl.BlockSpec((n_pieces, depth + PIECE_PAD, LANES), lambda i: (0, 0, 0), **once),
                any_spec, any_spec, any_spec,
                pl.BlockSpec((SUB, all_conv), lambda i: (seg_at(i), 0)),
                pl.BlockSpec((2, SUB, LANES), lambda i: (0, seg_at(i), 0)),
                pl.BlockSpec((SUB // SEG, n_state, inner_dim), lambda i: (seg_at(i), 0, 0)),
                pl.BlockSpec((LANES, inner_dim), lambda i: (0, 0), **once),
                pl.BlockSpec((1, inner_dim), lambda i: (0, 0)),
            ],
            out_specs=[
                pl.BlockSpec((1, half, group_inner), lambda i: (lax.rem(z_at(i), 2), 0, z_at(i) // 2)),
                pl.BlockSpec((SUB, inner_dim), lambda i: (seg_at(i), 0)),
                pl.BlockSpec((n_pieces, depth, LANES), lambda i: (0, 0, 0), **once),
            ],
            out_shape=[
                jax.ShapeDtypeStruct((2, half, inner_dim), BF16),
                jax.ShapeDtypeStruct((rows, inner_dim), F32),
                jax.ShapeDtypeStruct((n_pieces, depth, LANES), F32),
            ],
            scratch_shapes=[
                pltpu.VMEM((2, half, width), BF16),
                pltpu.VMEM((2, group_inner, width), BF16),
                pltpu.VMEM((n_pieces, depth + PIECE_PAD, LANES), F32),
                pltpu.VMEM((n_pieces, depth, LANES), F32),
                pltpu.VMEM((n_pieces, depth, LANES), F32),
                pltpu.SemaphoreType.DMA((2,)),
                pltpu.SemaphoreType.DMA((2,)),
                pltpu.SemaphoreType.DMA, pltpu.SemaphoreType.DMA,
                pltpu.SemaphoreType.DMA, pltpu.SemaphoreType.DMA,
            ],
            compiler_params=pltpu.CompilerParams(vmem_limit_bytes=limit, collective_id=0, has_side_effects=True),
            name="gate_ssd_exchange",
        )(end_state, tokens, other, w_in_t, act, dts, held, one_hot, skip_row)

        n_tiles = half // SUB

        def tile(i):
            return jnp.minimum(i, 2 * n_tiles - 1)

        def slot_of(i):
            return 1 - tile(i) // n_tiles

        def row_at(i):
            return lax.rem(lax.axis_index("tp") + slot_of(i), 2) * n_tiles + lax.rem(tile(i), n_tiles)

        def own_at(i):
            return jnp.maximum(i - n_tiles - 1, 0)

        def c_spec(g):
            return pl.BlockSpec((SUB, LANES), lambda i: (row_at(i), 6 * g + 5))

        return pl.pallas_call(
            functools.partial(gate_out_kernel, dims),
            grid=(2 * n_tiles + 1,),
            in_specs=[
                pl.BlockSpec((SUB, inner_dim), lambda i: (row_at(i), 0)),
                c_spec(0), c_spec(1), c_spec(2), c_spec(3),
                pl.BlockSpec((1, SUB, inner_dim), lambda i: (slot_of(i), lax.rem(tile(i), n_tiles), 0)),
                pl.BlockSpec((1, SUB, LANES), lambda i: (2, row_at(i), 0)),
                pl.BlockSpec((n_pieces, depth, LANES), lambda i: (0, 0, 0), **once),
                pl.BlockSpec((LANES, inner_dim), lambda i: (0, 0), **once),
                pl.BlockSpec((1, inner_dim), lambda i: (0, 0)),
                any_spec,
                pl.BlockSpec((SUB, width), lambda i: (own_at(i), 0)),
            ],
            out_specs=pl.BlockSpec((SUB, width), lambda i: (own_at(i), 0)),
            out_shape=jax.ShapeDtypeStruct((half, width), BF16),
            scratch_shapes=[
                pltpu.VMEM((inner_dim, width), BF16),
                pltpu.VMEM((n_state, inner_dim), BF16),
                pltpu.VMEM((SUB, inner_dim), BF16),
                pltpu.VMEM((SUB, inner_dim), BF16),
                pltpu.VMEM((n_tiles + 1, SUB, width), BF16),
                pltpu.VMEM((n_tiles, SUB, width), BF16),
                pltpu.SemaphoreType.DMA,
                pltpu.SemaphoreType.DMA((n_tiles,)),
                pltpu.SemaphoreType.DMA((n_tiles,)),
            ],
            compiler_params=pltpu.CompilerParams(vmem_limit_bytes=limit, **(dict(collective_id=1, has_side_effects=True) if EXCHANGE else {})),
            name="gate_out_swap",
        )(y_local, act, act, act, act, gate_z, dts, incoming, one_hot, norm_w[None], w_out, tokens)

    return jax.shard_map(
        layer_block,
        mesh=mesh,
        in_specs=(row_spec, P(None, "tp"), P(None, "tp", None), P("tp", None), P("tp"), P("tp"), P("tp"), P("tp"), P("tp", None)),
        out_specs=row_spec,
        check_vma=False)
```
